128 devices in a mesh: swath: 32 (over x, y, core), chan: 4 (over z).
Axes of the slice: x: 4, y: 4, z: 4, core: 2. Of those that a mesh axis runs over, the one named last changes fastest.
Arguments:
- innovations: float32 [2097152], P(('swath', 'chan')), may hold values from -6 to 6
- obs_precision: float32 [2097152], P(('swath', 'chan')), may hold values from 0.25 to 4
- jacobian: bfloat16 [2097152, 128], P(('swath', 'chan')), may hold values from -0.5 to 0.5
- predictors: float32 [8, 2097152], P(None, ('swath', 'chan')), may hold values from -5 to 5
- obs_column: int32 [2097152], P(('swath', 'chan')), may hold values from 0 to 2047, as said below
- obs_channel: int32 [2097152], P(('swath', 'chan')), may hold values from 0 to 5119
- obs_count: int32 [32, 4], P('swath', 'chan'), may hold values from 5461 to 16384, as said below
- smoothing: float32 [128], replicated, may hold values from 0.02 to 0.12
- bias_precision: float32 [8, 5120], P(None, 'chan'), may hold values from 1 to 100
Outputs:
- control_state: float32 [1024, 256, 128], P('swath', 'chan')
- bias_increment: float32 [8, 5120], P(None, 'chan')
- residual_norms: float32 [3], replicated
The draws below stay inside these ranges and needn't reach their ends.
Inputs may be any that keep to these rules, and one draw needn't show every extreme that they name: `obs_column`: Row-major index latitude row * 64 + longitude column within the tile of the device that holds the slot; all slots of an aligned block of 128 slots lie in one latitude row. `obs_channel`: channel c belongs to block c // 256, whose coefficients are owned by chan index c // 1280. `obs_count`: slots below the count hold live observations, the rest are ignored; some device is full in every draw.
All inputs are finite; a program needn't handle non-finite values.
Results may differ from the reference program's by a relative error of at most 0.0003.
Values sent between devices are 32-bit elements; how exact they have to be, the bound alone decides.
No kernel may reach another device: no remote copies, remote signals or barrier semaphores. Data moves between devices by JAX's collectives and lax.ppermute only.
A program may use at most 128 MiB of HBM per device.

```python
import math
import jax
import jax.numpy as jnp
from jax import lax

LEV = 128
NPRED = 8
OBS_BLOCK = 128
LAT_DEV = 32
LON_DEV = 64
OBS_DEV = 16384
ITERS = 2
OBS_ALL = 2097152
CHANNELS = 5120
N_SWATH = 32
N_CHAN = 4


def draw_obs_count(key, part):
    devices_all = N_SWATH * N_CHAN
    counts = jax.random.randint(jax.random.fold_in(key, 11), (devices_all,), OBS_DEV // 3, OBS_DEV + 1)
    fullest = jax.random.randint(jax.random.fold_in(key, 12), (), 0, devices_all)
    counts = jnp.where(jnp.arange(devices_all) == fullest, OBS_DEV, counts)
    return counts.reshape(N_SWATH, N_CHAN).astype(jnp.int32)


def draw_obs_column(key, part):
    block_count = OBS_DEV * N_SWATH * N_CHAN // OBS_BLOCK
    line_rows = jax.random.randint(jax.random.fold_in(key, 21), (block_count,), 0, LAT_DEV)
    line_cols = jax.random.randint(jax.random.fold_in(key, 22), (block_count, OBS_BLOCK), 0, LON_DEV)
    return (line_rows[:, None] * LON_DEV + line_cols).reshape(-1).astype(jnp.int32)


def touch_ends(entries, rng, smallest, largest):
    longest = entries.shape.index(max(entries.shape))
    spots = []
    for shift in (0, 1):
        where = [jax.random.randint(jax.random.fold_in(rng, axis), (), 0, length) for axis, length in enumerate(entries.shape)]
        where[longest] = (where[longest] + shift) % entries.shape[longest]
        spots.append(tuple(where))
    return entries.at[spots[0]].set(smallest).at[spots[1]].set(largest)


def steps_of(own_key, dims, split, least, top_value):
    def one(axis_at, blocks):
        draws = jax.random.uniform(jax.random.fold_in(jax.random.fold_in(own_key, 6), axis_at), (blocks,), jnp.float32, least / len(split), top_value / len(split))
        return jnp.repeat(jnp.exp(draws), dims[axis_at] // blocks).reshape((-1,) + (1,) * (len(dims) - axis_at - 1))

    level = one(*split[0])
    for cut in split[1:]:
        level = level * one(*cut)
    return level


def centred(own_key, shape, deviation, most, pieces=(), kind=jnp.bfloat16):
    result = jax.random.normal(own_key, shape, jnp.float32) * deviation
    if len(pieces) > 0:
        result = steps_of(own_key, shape, pieces, -0.22, 0.18) * result
    return jnp.clip(result, min=-most, max=most).astype(kind)


def setup_inputs(seed: int = 0) -> dict:
    arg_keys = jax.random.split(jax.random.key(seed), 10)
    innovations = centred(arg_keys[0], (OBS_ALL,), 1.0, 6.0, ((0, 128),), jnp.float32)
    obs_precision = jnp.clip(jnp.exp(math.log(4.0) - 2.7725887 * jax.random.uniform(arg_keys[1], (OBS_ALL,), jnp.float32) ** steps_of(arg_keys[1], (OBS_ALL,), ((0, 128),), -0.2, 0.2)), 0.25, 4.0)
    jacobian = centred(arg_keys[2], (OBS_ALL, LEV), LEV ** -0.5, 0.5, ((0, 128),))
    predictors = centred(arg_keys[3], (NPRED, OBS_ALL), 1.0, 5.0, ((1, 128),), jnp.float32)
    obs_column = draw_obs_column(jax.random.fold_in(arg_keys[9], 71), 0)
    obs_channel = touch_ends(jax.random.randint(arg_keys[5], (OBS_ALL,), 0, CHANNELS), jax.random.fold_in(arg_keys[5], 1), 0, CHANNELS - 1).astype(jnp.int32)
    obs_count = draw_obs_count(jax.random.fold_in(arg_keys[9], 71), 0)
    smoothing = jnp.clip(jnp.exp(jax.random.uniform(arg_keys[7], (LEV,), jnp.float32, math.log(0.02), math.log(0.12))), 0.02, 0.12)
    bias_precision = jnp.clip(jnp.exp(math.log(100.0) - 4.6051702 * jax.random.uniform(arg_keys[8], (NPRED, CHANNELS), jnp.float32) ** steps_of(arg_keys[8], (NPRED, CHANNELS), ((1, 4),), -0.2, 0.2)), 1.0, 100.0)
    return dict(innovations=innovations, obs_precision=obs_precision, jacobian=jacobian, predictors=predictors, obs_column=obs_column, obs_channel=obs_channel, obs_count=obs_count, smoothing=smoothing, bias_precision=bias_precision)


def smooth_field(state_field, smoothing):
    padded = jnp.pad(state_field, ((1, 1), (0, 0), (0, 0)))
    beside = padded[:-2] + padded[2:] + jnp.roll(state_field, 1, axis=1) + jnp.roll(state_field, -1, axis=1)
    return state_field + smoothing * (beside - 4.0 * state_field)

def reference(innovations, obs_precision, jacobian, predictors, obs_column, obs_channel, obs_count, smoothing, bias_precision):
    devices_all = N_SWATH * N_CHAN
    lat_all = LAT_DEV * N_SWATH
    lon_all = LON_DEV * N_CHAN
    cells_all = lat_all * lon_all
    slot_ids = jnp.arange(devices_all * OBS_DEV, dtype=jnp.int32)
    holder = slot_ids // OBS_DEV
    row_index = holder // N_CHAN * LAT_DEV + obs_column // LON_DEV
    col_index = holder % N_CHAN * LON_DEV + obs_column % LON_DEV
    flat_cell = (row_index * lon_all + col_index).astype(jnp.int32)
    live = slot_ids % OBS_DEV < obs_count.reshape(-1)[holder]
    weights = jnp.where(live, obs_precision, jnp.zeros_like(obs_precision))
    jac_blocks = jacobian.reshape(devices_all, OBS_DEV, LEV)
    cell_blocks = flat_cell.reshape(devices_all, OBS_DEV)

    def forward(state_field):
        table = state_field.reshape(cells_all, LEV)

        def one_block(pair):
            return lax.optimization_barrier(jnp.sum(pair[0].astype(jnp.float32) * table[pair[1]], axis=1))
        return lax.map(one_block, (jac_blocks, cell_blocks)).reshape(-1)

    def adjoint(values):
        value_blocks = values.reshape(devices_all, OBS_DEV)

        def add_block(table, triple):
            return (table.at[triple[1]].add(triple[0].astype(jnp.float32) * triple[2][:, None]), 0)
        start_table = jnp.zeros((cells_all, LEV), jnp.float32)
        table = lax.scan(add_block, start_table, (jac_blocks, cell_blocks, value_blocks))[0]
        return table.reshape(lat_all, lon_all, LEV)

    def bias_forward(coefs):
        return lax.optimization_barrier(jnp.sum(predictors * coefs[:, obs_channel], axis=0))

    def bias_adjoint(terms):
        return jnp.zeros((NPRED, CHANNELS), jnp.float32).at[:, obs_channel].add(terms)

    def hessian(state_dir, bias_dir):
        image = weights * (forward(smooth_field(state_dir, smoothing)) + bias_forward(bias_dir))
        return (state_dir + smooth_field(adjoint(image), smoothing), bias_precision * bias_dir + bias_adjoint(predictors * image[None, :]))
    source = weights * innovations
    res_state = smooth_field(adjoint(source), smoothing)
    res_bias = bias_adjoint(predictors * source[None, :])
    diagonal = bias_precision + bias_adjoint(predictors * predictors * weights[None, :])
    sol_state = jnp.zeros_like(res_state)
    sol_bias = jnp.zeros_like(res_bias)
    pre_bias = res_bias / diagonal
    dir_state, dir_bias = (res_state, pre_bias)
    state_sq = jnp.sum(res_state * res_state)
    rz_now = state_sq + jnp.sum(res_bias * pre_bias)
    record = [state_sq + jnp.sum(res_bias * res_bias)]
    for turn_index in range(ITERS):
        img_state, img_bias = hessian(dir_state, dir_bias)
        length = rz_now / (jnp.sum(dir_state * img_state) + jnp.sum(dir_bias * img_bias))
        sol_state = sol_state + length * dir_state
        sol_bias = sol_bias + length * dir_bias
        res_state = res_state - length * img_state
        res_bias = res_bias - length * img_bias
        pre_bias = res_bias / diagonal
        state_sq = jnp.sum(res_state * res_state)
        rz_next = state_sq + jnp.sum(res_bias * pre_bias)
        record.append(state_sq + jnp.sum(res_bias * res_bias))
        ratio = rz_next / rz_now
        dir_state = res_state + ratio * dir_state
        dir_bias = pre_bias + ratio * dir_bias
        rz_now = rz_next
    return (sol_state, sol_bias, jnp.sqrt(jnp.stack(record)))
```

```python
import functools

import jax
import jax.numpy as jnp
from jax import lax
from jax.experimental import pallas as pl
from jax.experimental.pallas import tpu as pltpu
from jax.sharding import Mesh
from jax.sharding import PartitionSpec as P

LEV = 128
NPRED = 8
LINE = 128
LAT_DEV = 32
LON_DEV = 64
SLOTS = 16384
LINES = SLOTS // LINE
GROUP = 8
KSLOT = GROUP * LINE
LOW = 256
HIGH = 20
CHAN_HIGH = 5
PAD_HIGH = 6
ROWS = 3
DEVICES = 128
TABLE = DEVICES * ROWS
SWATH = ("swath_0", "swath_1", "swath_2")
SWATH_CHAN = ("swath_0", "swath_1", "swath_2", "chan")
OWNERS = ("chan", "swath_0", "swath_1", "swath_2")
F32 = jnp.float32
BF16 = jnp.bfloat16

VMEM = pl.BlockSpec(memory_space=pltpu.VMEM)
SMEM = pl.BlockSpec(memory_space=pltpu.SMEM)


def call(kernel, out_shape, in_specs, args, scratch=(), flops=10**9, limit=40, name=None):
    outs = out_shape if isinstance(out_shape, (tuple, list)) else [out_shape]
    return pl.pallas_call(
        kernel,
        out_shape=out_shape,
        in_specs=in_specs,
        out_specs=jax.tree.map(lambda _: VMEM, out_shape),
        scratch_shapes=list(scratch),
        compiler_params=pltpu.CompilerParams(vmem_limit_bytes=limit * 2**20),
        cost_estimate=pl.CostEstimate(flops=flops, bytes_accessed=4 * 2**20, transcendentals=0),
        name=name,
    )(*args)


def split(x):
    high = x.astype(BF16)
    return high, (x - high.astype(F32)).astype(BF16)


def slot_of(high):
    return high // CHAN_HIGH * PAD_HIGH + high % CHAN_HIGH


def one_hot_low(low8, hot_ref):
    ids = lax.broadcasted_iota(jnp.int32, (LOW, LINE), 0).astype(F32).astype(BF16)
    low = low8.astype(F32)
    for j in range(GROUP):
        row = jnp.broadcast_to(low[j : j + 1], (LOW, LINE)).astype(BF16)
        hot_ref[:, j * LINE : (j + 1) * LINE] = jnp.where(
            ids == row, jnp.ones((), BF16), jnp.zeros((), BF16)
        )


def spread_high(values, high_row, parts):
    offset = (lax.broadcasted_iota(jnp.int32, (16, LINE), 0) // 8).astype(F32)
    base = (jnp.broadcast_to(high_row, (16, LINE)) - offset).astype(BF16)
    pieces = []
    for value in values:
        for half in split(value):
            pieces.append(jnp.concatenate([half, half], axis=0))
    for m in range(HIGH // 2):
        mask = base == jnp.array(2 * m, BF16)
        for piece, (ref, cols) in zip(pieces, parts):
            ref[16 * m : 16 * m + 16, cols] = jnp.where(mask, piece, jnp.zeros((), BF16))


def dot_rows(left, right):
    return lax.dot_general(left, right, (((1,), (1,)), ((), ())), preferred_element_type=F32)


def table_start_kernel(
    count_ref, innov_ref, prec_ref, pred_ref, chan_ref,
    table_ref, weight_ref, source_ref,
    hot_ref, a_hi, a_lo, b_hi, b_lo, acc_ref, acc2_ref,
):
    count = count_ref[0, 0]
    acc_ref[...] = jnp.zeros_like(acc_ref)
    acc2_ref[...] = jnp.zeros_like(acc2_ref)

    def step(g, _):
        rows = pl.ds(pl.multiple_of(g * GROUP, GROUP), GROUP)
        slot = (
            g * KSLOT
            + lax.broadcasted_iota(jnp.int32, (GROUP, LINE), 0) * LINE
            + lax.broadcasted_iota(jnp.int32, (GROUP, LINE), 1)
        )
        weight = jnp.where(slot < count, prec_ref[rows, :], 0.0)
        source = weight * innov_ref[rows, :]
        weight_ref[rows, :] = weight
        source_ref[rows, :] = source
        chan = chan_ref[rows, :]
        one_hot_low(chan & (LOW - 1), hot_ref)
        high = (chan >> 8).astype(F32)
        for j in range(GROUP):
            pred = pred_ref[:, pl.ds(pl.multiple_of(g * KSLOT + j * LINE, LINE), LINE)]
            cols = slice(j * LINE, (j + 1) * LINE)
            spread_high(
                [pred * source[j : j + 1], pred * pred * weight[j : j + 1]],
                high[j : j + 1],
                [(a_hi, cols), (a_lo, cols), (b_hi, cols), (b_lo, cols)],
            )
        hot = hot_ref[...]
        acc_ref[...] += dot_rows(a_hi[...], hot) + dot_rows(a_lo[...], hot)
        acc2_ref[...] += dot_rows(b_hi[...], hot) + dot_rows(b_lo[...], hot)
        return 0

    lax.fori_loop(0, LINES // GROUP, step, 0)
    table_ref[...] = jnp.zeros_like(table_ref)
    for high in range(HIGH):
        for half in range(2):
            at = 16 * (slot_of(high) * 2 + half)
            cols = slice(half * 128, half * 128 + 128)
            table_ref[pl.ds(at, 8, stride=2), :] = acc_ref[high * 8 : high * 8 + 8, cols]
            table_ref[pl.ds(at + 1, 8, stride=2), :] = acc2_ref[high * 8 : high * 8 + 8, cols]


def image_kernel(
    coef_ref, weight_ref, state_ref, pred_ref, chan_ref,
    table_ref, image_ref,
    hot_ref, got_ref, c_hi, c_lo, a_hi, a_lo, acc_ref,
):
    for high in range(HIGH):
        for half in range(2):
            at = 8 * (slot_of(high) * 2 + half)
            acc_ref[high * 8 : high * 8 + 8, half * 128 : half * 128 + 128] = coef_ref[at : at + 8, :]
    high_part, low_part = split(acc_ref[...])
    c_hi[...] = high_part
    c_lo[...] = low_part
    acc_ref[...] = jnp.zeros_like(acc_ref)

    def step(g, _):
        rows = pl.ds(pl.multiple_of(g * GROUP, GROUP), GROUP)
        chan = chan_ref[rows, :]
        one_hot_low(chan & (LOW - 1), hot_ref)
        hot = hot_ref[...]
        got_ref[...] = jnp.dot(c_hi[...], hot, preferred_element_type=F32) + jnp.dot(
            c_lo[...], hot, preferred_element_type=F32
        )
        high_id = chan >> 8
        looked = []
        preds = []
        for j in range(GROUP):
            cols = slice(j * LINE, (j + 1) * LINE)
            pred = pred_ref[:, pl.ds(pl.multiple_of(g * KSLOT + j * LINE, LINE), LINE)]
            ids = jnp.broadcast_to(high_id[j : j + 1], (8, LINE))
            coef = got_ref[0:8, cols]
            for high in range(1, HIGH):
                coef = jnp.where(ids == high, got_ref[high * 8 : high * 8 + 8, cols], coef)
            looked.append(jnp.sum(pred * coef, axis=0, keepdims=True))
            preds.append(pred)
        image = weight_ref[rows, :] * (state_ref[rows, :] + jnp.concatenate(looked, axis=0))
        image_ref[rows, :] = image
        high_f = high_id.astype(F32)
        for j in range(GROUP):
            cols = slice(j * LINE, (j + 1) * LINE)
            spread_high(
                [preds[j] * image[j : j + 1]], high_f[j : j + 1], [(a_hi, cols), (a_lo, cols)]
            )
        acc_ref[...] += dot_rows(a_hi[...], hot) + dot_rows(a_lo[...], hot)
        return 0

    lax.fori_loop(0, LINES // GROUP, step, 0)
    table_ref[...] = jnp.zeros_like(table_ref)
    for high in range(HIGH):
        for half in range(2):
            at = 8 * (slot_of(high) * 2 + half)
            table_ref[at : at + 8, :] = acc_ref[
                high * 8 : high * 8 + 8, half * 128 : half * 128 + 128
            ]


def adjoint_kernel(row_ref, col_ref, value_ref, jac_ref, field_ref):
    field_ref[...] = jnp.zeros_like(field_ref)
    ids = lax.broadcasted_iota(jnp.int32, (LON_DEV, LINE), 0).astype(F32).astype(BF16)

    def step(g, _):
        rows = pl.ds(pl.multiple_of(g * GROUP, GROUP), GROUP)
        col = col_ref[rows, :].astype(F32)
        value = value_ref[rows, :]
        high = value.astype(BF16).astype(F32)
        low = value - high
        for j in range(GROUP):
            mask = ids == jnp.broadcast_to(col[j : j + 1], (LON_DEV, LINE)).astype(BF16)
            hot_hi = jnp.where(
                mask, jnp.broadcast_to(high[j : j + 1], (LON_DEV, LINE)).astype(BF16), jnp.zeros((), BF16)
            )
            hot_lo = jnp.where(
                mask, jnp.broadcast_to(low[j : j + 1], (LON_DEV, LINE)).astype(BF16), jnp.zeros((), BF16)
            )
            jac = jac_ref[pl.ds(pl.multiple_of(g * KSLOT + j * LINE, LINE), LINE), :]
            add = jnp.dot(hot_hi, jac, preferred_element_type=F32) + jnp.dot(
                hot_lo, jac, preferred_element_type=F32
            )
            at = row_ref[g * GROUP + j]
            field_ref[at] += add
        return 0

    lax.fori_loop(0, LINES // GROUP, step, 0)


def smoothed_row(mid, above, below, smoothing, size):
    left = pltpu.roll(mid, 1, 0)
    right = pltpu.roll(mid, size - 1, 0)
    return mid + smoothing * (above + below + left + right - 4.0 * mid)


WIDE = LON_DEV + 16


def forward_kernel(
    row_ref, edge_ref, field_ref, north_ref, south_ref, west_ref, east_ref, smooth_ref, col_ref, jac_ref,
    out_ref, seen_ref,
    ext_ref, mid_ref, f_hi, f_lo,
):
    ext_ref[...] = jnp.zeros_like(ext_ref)
    ext_ref[2 : LAT_DEV + 2, 8 : 8 + LON_DEV] = field_ref[...]
    ext_ref[0:2, 8 : 8 + LON_DEV] = north_ref[...]
    ext_ref[LAT_DEV + 2 : LAT_DEV + 4, 8 : 8 + LON_DEV] = south_ref[...]
    ext_ref[:, 6:8] = west_ref[...]
    ext_ref[:, 8 + LON_DEV : 10 + LON_DEV] = east_ref[...]
    smoothing = smooth_ref[...]

    def first(r, _):
        mid_ref[r] = smoothed_row(ext_ref[r + 1], ext_ref[r], ext_ref[r + 2], smoothing, WIDE)
        return 0

    lax.fori_loop(0, LAT_DEV + 2, first, 0)
    mid_ref[0] = mid_ref[0] * jnp.where(edge_ref[0] > 0, 1.0, 0.0)
    mid_ref[LAT_DEV + 1] = mid_ref[LAT_DEV + 1] * jnp.where(edge_ref[1] > 0, 1.0, 0.0)

    def second(r, _):
        mid = mid_ref[r + 1]
        twice = smoothed_row(mid, mid_ref[r], mid_ref[r + 2], smoothing, WIDE)
        out_ref[r] = mid[8 : 8 + LON_DEV]
        high, low = split(twice[8 : 8 + LON_DEV])
        f_hi[r] = high
        f_lo[r] = low
        return 0

    lax.fori_loop(0, LAT_DEV, second, 0)
    ids = lax.broadcasted_iota(jnp.int32, (LON_DEV, LINE), 0)

    def step(g, _):
        rows = pl.ds(pl.multiple_of(g * GROUP, GROUP), GROUP)
        col = col_ref[rows, :]
        seen = []
        for j in range(GROUP):
            jac = jac_ref[pl.ds(pl.multiple_of(g * KSLOT + j * LINE, LINE), LINE), :]
            at = row_ref[g * GROUP + j]
            grid = dot_rows(f_hi[at], jac) + dot_rows(f_lo[at], jac)
            mask = ids == jnp.broadcast_to(col[j : j + 1], (LON_DEV, LINE))
            seen.append(jnp.sum(jnp.where(mask, grid, 0.0), axis=0, keepdims=True))
        seen_ref[rows, :] = jnp.concatenate(seen, axis=0)
        return 0

    lax.fori_loop(0, LINES // GROUP, step, 0)


def lanes_of(values):
    lane = lax.broadcasted_iota(jnp.int32, (1, 128), 1)
    row = jnp.zeros((1, 128), F32)
    for i, value in enumerate(values):
        row = jnp.where(lane == i, value, row)
    return row


def total(x):
    return jnp.sum(jnp.sum(x, axis=0, keepdims=True), axis=1, keepdims=True)


def state_sums_kernel(
    field_ref, north_ref, south_ref, west_ref, east_ref, smooth_ref,
    source_ref, image1_ref, image2_ref, seen1_ref, seen2_ref,
    sums_ref,
    ext_ref,
):
    ext_ref[...] = jnp.zeros_like(ext_ref)
    ext_ref[1 : LAT_DEV + 1, 8 : 8 + LON_DEV] = field_ref[...]
    ext_ref[0:1, 8 : 8 + LON_DEV] = north_ref[...]
    ext_ref[LAT_DEV + 1 : LAT_DEV + 2, 8 : 8 + LON_DEV] = south_ref[...]
    ext_ref[1 : LAT_DEV + 1, 7:8] = west_ref[...]
    ext_ref[1 : LAT_DEV + 1, 8 + LON_DEV : 9 + LON_DEV] = east_ref[...]
    smoothing = smooth_ref[...]

    def first(r, acc):
        row = smoothed_row(ext_ref[r + 1], ext_ref[r], ext_ref[r + 2], smoothing, WIDE)
        row = row[8 : 8 + LON_DEV]
        return acc + row * row

    acc = lax.fori_loop(0, LAT_DEV, first, jnp.zeros((LON_DEV, LEV), F32))
    source, image1, image2 = (source_ref[...], image1_ref[...], image2_ref[...])
    seen1, seen2 = (seen1_ref[...], seen2_ref[...])
    sums_ref[...] = lanes_of(
        [
            total(seen1 * source),
            total(seen1 * image1),
            total(seen2 * image1),
            total(seen1 * image2),
            total(seen2 * image2),
            total(acc),
        ]
    )


def arrived_sum(ref, rows):
    acc = ref[0:24, :]
    for g in range(1, ref.shape[0] // 24):
        acc = acc + ref[24 * g : 24 * g + 24, :]
    out = acc[0:rows]
    for s in range(1, 24 // rows):
        out = out + acc[rows * s : rows * s + rows]
    return out


def to_everyone(rows, ref):
    tile = jnp.concatenate([rows] * (24 // rows.shape[0]), axis=0)
    for g in range(ref.shape[0] // 24):
        ref[24 * g : 24 * g + 24, :] = tile


def owner_start_kernel(arrived_ref, prior_ref, out_ref, own_ref):
    both = arrived_sum(arrived_ref, 2 * ROWS)
    res = jnp.concatenate([both[2 * i : 2 * i + 1] for i in range(ROWS)], axis=0)
    diag = jnp.concatenate([both[2 * i + 1 : 2 * i + 2] for i in range(ROWS)], axis=0)
    diag = diag + prior_ref[...]
    pre = res / diag
    own_ref[0:3] = res
    own_ref[3:6] = pre
    own_ref[6:9] = diag
    to_everyone(pre, out_ref)


def owner_next_kernel(arrived_ref, prior_ref, own_ref, out_ref, next_ref):
    image = arrived_sum(arrived_ref, ROWS) + prior_ref[...] * own_ref[3:6]
    pre = image / own_ref[6:9]
    next_ref[0:3] = image
    next_ref[3:6] = pre
    to_everyone(pre, out_ref)


def owner_last_kernel(arrived_ref, prior_ref, own_ref, next_ref, sums_ref, out_ref):
    res, pre = (own_ref[0:3], own_ref[3:6])
    image, image_pre = (next_ref[0:3], next_ref[3:6])
    last = arrived_sum(arrived_ref, ROWS) + prior_ref[...] * image_pre
    row = lanes_of(
        [jnp.zeros((1, 1), F32)] * 6
        + [
            total(res * pre),
            total(res * res),
            total(pre * image),
            total(image * image_pre),
            total(res * image),
            total(image * image),
            total(image_pre * last),
            total(res * last),
            total(image * last),
            total(last * last),
        ]
    )
    out_ref[...] = jnp.broadcast_to(row + sums_ref[...], out_ref.shape)


def finish_kernel(chan_ref, arrived_ref, a_ref, b_ref, pre_ref, image_pre_ref, x_ref, bias_ref, norm_ref):
    sums = jnp.sum(arrived_ref[...], axis=0, keepdims=True)
    lane = lax.broadcasted_iota(jnp.int32, (1, 128), 1)
    pick = [
        jnp.sum(jnp.where(lane == i, sums, 0.0), axis=1, keepdims=True) for i in range(16)
    ]
    aa, ab, bb, ac, bc, cc = pick[:6]
    rz_b, rr_b, zq_b, qw_b, rq_b, qq_b, wt_b, rt_b, qt_b, tt_b = pick[6:]
    state_qq = aa + 2.0 * ab + bb
    state_qc = ac + bc
    rz0 = aa + rz_b
    rr0 = aa + rr_b
    zq = aa + ab + zq_b
    qw = state_qq + qw_b
    rq = aa + ab + rq_b
    qq = state_qq + qq_b
    wt = state_qq + state_qc + wt_b
    rt = aa + ab + ac + rt_b
    qt = state_qq + state_qc + qt_b
    tt = state_qq + 2.0 * state_qc + cc + tt_b
    alpha0 = rz0 / zq
    rz1 = rz0 - 2.0 * alpha0 * zq + alpha0 * alpha0 * qw
    rr1 = rr0 - 2.0 * alpha0 * rq + alpha0 * alpha0 * qq
    beta = rz1 / rz0
    grow = 1.0 + beta
    pq = grow * grow * zq - 2.0 * alpha0 * grow * qw + alpha0 * alpha0 * wt
    alpha1 = rz1 / pq
    along = alpha0 + alpha1 * grow
    back = alpha0 * alpha1
    rr2 = (
        rr0
        - 2.0 * along * rq
        + 2.0 * back * rt
        + along * along * qq
        - 2.0 * along * back * qt
        + back * back * tt
    )
    norm_ref[...] = jnp.sqrt(jnp.maximum(lanes_of([rr0, rr1, rr2]), 0.0))
    coef_a = along - back
    x_ref[...] = coef_a[None] * a_ref[...] - back[None] * b_ref[...]
    start = chan_ref[0] * (PAD_HIGH * 16)
    for i in range(2 * CHAN_HIGH):
        rows = pl.ds(pl.multiple_of(start + 8 * i, 8), 8)
        bias_ref[:, 128 * i : 128 * i + 128] = along * pre_ref[rows, :] - back * image_pre_ref[rows, :]


def exchange(array, width):
    moved = lax.all_to_all(
        array.reshape(DEVICES, 1, width), OWNERS, split_axis=0, concat_axis=0, tiled=True
    )
    return moved.reshape(array.shape)


def halo(field, width):
    bands = lax.axis_size(SWATH)
    sectors = lax.axis_size("chan")
    north = lax.ppermute(field[LAT_DEV - width :], SWATH, [(i, i + 1) for i in range(bands - 1)])
    south = lax.ppermute(field[:width], SWATH, [(i + 1, i) for i in range(bands - 1)])

    def columns(part):
        if width == 1:
            return part(field)
        return jnp.concatenate([part(north), part(field), part(south)], axis=0)

    ring = [(i, (i + 1) % sectors) for i in range(sectors)]
    west = lax.ppermute(columns(lambda f: f[:, LON_DEV - width :]), "chan", ring)
    east = lax.ppermute(columns(lambda f: f[:, :width]), "chan", [(b, a) for a, b in ring])
    return north, south, west, east


def shape(*dims):
    return jax.ShapeDtypeStruct(dims, F32)


def body(
    innovations,
    obs_precision,
    jacobian,
    predictors,
    obs_column,
    obs_channel,
    obs_count,
    smoothing,
    bias_precision,
):
    band = lax.axis_index(SWATH)
    sector = lax.axis_index("chan")
    square = (LINES, LINE)
    chan = obs_channel.reshape(square)
    col_all = obs_column.reshape(square)
    line_row = col_all[:, 0] // LON_DEV
    col = col_all % LON_DEV
    smooth = smoothing.reshape(1, LEV)
    edges = jnp.stack([band > 0, band < lax.axis_size(SWATH) - 1]).astype(jnp.int32)
    prior = bias_precision.reshape(NPRED, 2 * CHAN_HIGH, 128).transpose(1, 0, 2).reshape(-1, 128)
    prior = jnp.pad(prior, ((0, 16), (0, 0)), constant_values=1.0)
    prior = lax.dynamic_slice_in_dim(prior, band * ROWS, ROWS, axis=0)
    field_shape = shape(LAT_DEV, LON_DEV, LEV)
    spread = pltpu.VMEM((HIGH * 8, KSLOT), BF16)
    table_acc = pltpu.VMEM((HIGH * 8, LOW), F32)
    hot = pltpu.VMEM((LOW, KSLOT), BF16)

    table0, weights, source = call(
        table_start_kernel,
        (shape(2 * TABLE, 128), shape(*square), shape(*square)),
        [SMEM] + [VMEM] * 4,
        (obs_count, innovations.reshape(square), obs_precision.reshape(square), predictors, chan),
        [hot, spread, spread, spread, spread, table_acc, table_acc],
        flops=4 * 10**9,
        name="table_start",
    )

    def adjoint(values):
        return call(
            adjoint_kernel,
            field_shape,
            [SMEM] + [VMEM] * 3,
            (line_row, col, values, jacobian),
            flops=2 * 10**9,
            name="adjoint",
        )

    def forward(field):
        wide = pltpu.VMEM((LAT_DEV + 4, WIDE, LEV), F32)
        mid = pltpu.VMEM((LAT_DEV + 2, WIDE, LEV), F32)
        half = pltpu.VMEM((LAT_DEV, LON_DEV, LEV), BF16)
        return call(
            forward_kernel,
            (field_shape, shape(*square)),
            [SMEM, SMEM] + [VMEM] * 8,
            (line_row, edges, field, *halo(field, 2), smooth, col, jacobian),
            [wide, mid, half, half],
            flops=2 * 10**9,
            name="forward",
        )

    def image_of(coefs, state):
        return call(
            image_kernel,
            (shape(TABLE, 128), shape(*square)),
            [VMEM] * 5,
            (coefs, weights, state, predictors, chan),
            [
                hot,
                pltpu.VMEM((HIGH * 8, KSLOT), F32),
                pltpu.VMEM((HIGH * 8, LOW), BF16),
                pltpu.VMEM((HIGH * 8, LOW), BF16),
                spread,
                spread,
                table_acc,
            ],
            flops=4 * 10**9,
            name="image",
        )

    arrived0 = exchange(table0, 2 * ROWS * 128)
    send0, own = call(
        owner_start_kernel, (shape(TABLE, 128), shape(9, 128)), [VMEM] * 2, (arrived0, prior), name="owner_start"
    )
    pre = exchange(send0, ROWS * 128)
    a_field, seen1 = forward(adjoint(source))
    table1, image1 = image_of(pre, seen1)
    arrived1 = exchange(table1, ROWS * 128)
    send1, own_next = call(
        owner_next_kernel, (shape(TABLE, 128), shape(6, 128)), [VMEM] * 3, (arrived1, prior, own), name="owner_next"
    )
    image_pre = exchange(send1, ROWS * 128)
    b_field, seen2 = forward(adjoint(image1))
    table2, image2 = image_of(image_pre, seen1 + seen2)
    arrived2 = exchange(table2, ROWS * 128)
    last = adjoint(image2)
    sums = call(
        state_sums_kernel,
        shape(1, 128),
        [VMEM] * 11,
        (last, *halo(last, 1), smooth, source, image1, image2, seen1, seen2),
        [pltpu.VMEM((LAT_DEV + 2, WIDE, LEV), F32)],
        name="state_sums",
    )
    send2 = call(
        owner_last_kernel,
        shape(DEVICES, 128),
        [VMEM] * 5,
        (arrived2, prior, own, own_next, sums),
        name="owner_last",
    )
    arrived3 = exchange(send2, 128)
    state, bias, norms = call(
        finish_kernel,
        (field_shape, shape(NPRED, 2 * CHAN_HIGH * 128), shape(1, 128)),
        [SMEM] + [VMEM] * 5,
        (sector.reshape(1), arrived3, a_field, b_field, pre, image_pre),
        name="finish",
    )
    return state, bias, norms[0, :3]


def solution(mesh):
    torus = Mesh(
        mesh.devices.reshape(4, 4, 2, mesh.shape["chan"]), ("swath_0", "swath_1", "swath_2", "chan")
    )
    placed = (
        P(SWATH_CHAN),
        P(SWATH_CHAN),
        P(SWATH_CHAN, None),
        P(None, SWATH_CHAN),
        P(SWATH_CHAN),
        P(SWATH_CHAN),
        P(SWATH, "chan"),
        P(),
        P(None, "chan"),
    )
    return jax.shard_map(
        body,
        mesh=torus,
        in_specs=placed,
        out_specs=(P(SWATH, "chan", None), P(None, "chan"), P()),
        check_vma=False,
    )
```

```python
import functools

import jax
import jax.numpy as jnp
from jax import lax
from jax.experimental import pallas as pl
from jax.experimental.pallas import tpu as pltpu
from jax.sharding import Mesh
from jax.sharding import PartitionSpec as P

LEV = 128
NPRED = 8
LINE = 128
LAT_DEV = 32
LON_DEV = 64
SLOTS = 16384
LINES = SLOTS // LINE
GROUP = 8
KSLOT = GROUP * LINE
SUBS = 8
UNROLL = 32
STAGES = LINES // UNROLL
LOW = 256
HIGH = 20
CHAN_HIGH = 5
N_BLOCK = 4
ROWS = 3
DEVICES = 128
TABLE = DEVICES * ROWS
SWATH = ("swath_0", "swath_1", "swath_2")
SWATH_CHAN = ("swath_0", "swath_1", "swath_2", "chan")
F32 = jnp.float32
BF16 = jnp.bfloat16

VMEM = pl.BlockSpec(memory_space=pltpu.VMEM)
SMEM = pl.BlockSpec(memory_space=pltpu.SMEM)
HBM = pl.BlockSpec(memory_space=pltpu.HBM)


def call(kernel, out_shape, in_specs, args, scratch=(), flops=10**9, limit=40, name=None, outs=None):
    return pl.pallas_call(
        kernel,
        out_shape=out_shape,
        in_specs=in_specs,
        out_specs=outs or jax.tree.map(lambda _: VMEM, out_shape),
        scratch_shapes=list(scratch),
        compiler_params=pltpu.CompilerParams(vmem_limit_bytes=int(limit * 2**20)),
        cost_estimate=pl.CostEstimate(flops=flops, bytes_accessed=4 * 2**20, transcendentals=0),
        name=name,
    )(*args)


def split(x):
    high = x.astype(BF16)
    return high, (x - high.astype(F32)).astype(BF16)


def table_tiles():
    for high in range(HIGH):
        for half in range(2):
            tile = high % CHAN_HIGH * 2 + half
            yield high, half, high // CHAN_HIGH, tile


def tile_rows(block, tile, rows, offset=0):
    start = N_BLOCK * rows * 8 * (tile % 4) + rows * block + tile // 4 + offset
    return pl.ds(start, 8, stride=N_BLOCK * rows)


def one_hot_low(low8, hot_ref):
    ids = lax.broadcasted_iota(jnp.int32, (LOW, LINE), 0).astype(F32).astype(BF16)
    low = low8.astype(F32)
    for j in range(GROUP):
        row = jnp.broadcast_to(low[j : j + 1], (LOW, LINE)).astype(BF16)
        hot_ref[:, j * LINE : (j + 1) * LINE] = jnp.where(
            ids == row, jnp.ones((), BF16), jnp.zeros((), BF16)
        )


def joined(ref, part, high, cols):
    at = 8 * HIGH * part + 8 * high
    return ref[at : at + 8, cols] + ref[at + 8 * HIGH : at + 8 * HIGH + 8, cols]


def spread_high(values, high_row, spread_ref, cols):
    offset = (lax.broadcasted_iota(jnp.int32, (16, LINE), 0) // 8).astype(F32)
    base = (jnp.broadcast_to(high_row, (16, LINE)) - offset).astype(BF16)
    pieces = []
    for value in values:
        for half in split(value):
            pieces.append(jnp.concatenate([half, half], axis=0))
    for m in range(HIGH // 2):
        mask = base == jnp.array(2 * m, BF16)
        for i, piece in enumerate(pieces):
            at = 8 * HIGH * i + 16 * m
            spread_ref[at : at + 16, cols] = jnp.where(mask, piece, jnp.zeros((), BF16))


def dot_rows(left, right):
    return lax.dot_general(left, right, (((1,), (1,)), ((), ())), preferred_element_type=F32)


def live_weights(count, g, lines, prec):
    slot = (
        g * lines * LINE
        + lax.broadcasted_iota(jnp.int32, (lines, LINE), 0) * LINE
        + lax.broadcasted_iota(jnp.int32, (lines, LINE), 1)
    )
    return jnp.where(slot < count, prec, 0.0)


def table_start_kernel(
    count_ref, innov_hbm, prec_hbm, pred_hbm, chan_hbm,
    table_ref,
    innov_ref, prec_ref, pred_ref, chan_ref, sems,
    hot_ref, spread_ref, acc_ref,
):
    small = [
        pltpu.make_async_copy(source, target, sems.at[i])
        for i, (source, target) in enumerate(
            [(chan_hbm, chan_ref), (innov_hbm, innov_ref), (prec_hbm, prec_ref)]
        )
    ]

    def large(i):
        at = pl.ds(pl.multiple_of(i * SUBS * KSLOT, SUBS * KSLOT), SUBS * KSLOT)
        return pltpu.make_async_copy(pred_hbm.at[:, at], pred_ref.at[:, at], sems.at[3 + i])

    steps = LINES // GROUP // SUBS
    for copy in small + [large(i) for i in range(steps)]:
        copy.start()
    count = count_ref[0, 0]
    acc_ref[...] = jnp.zeros_like(acc_ref)
    table_ref[...] = jnp.zeros_like(table_ref)
    for copy in small:
        copy.wait()

    def prepare(g, sub):
        rows = pl.ds(pl.multiple_of(g * GROUP, GROUP), GROUP)
        weight = live_weights(count, g, GROUP, prec_ref[rows, :])
        source = weight * innov_ref[rows, :]
        chan = chan_ref[rows, :]
        one_hot_low(chan & (LOW - 1), hot_ref.at[sub])
        high = (chan >> 8).astype(F32)
        for j in range(GROUP):
            pred = pred_ref[:, pl.ds(pl.multiple_of(g * KSLOT + j * LINE, LINE), LINE)]
            spread_high(
                [pred * source[j : j + 1], pred * pred * weight[j : j + 1]],
                high[j : j + 1],
                spread_ref.at[sub],
                slice(j * LINE, (j + 1) * LINE),
            )

    def step(i, _):
        large(i).wait()
        for sub in range(SUBS):
            prepare(i * SUBS + sub, sub)
        acc = dot_rows(spread_ref[0], hot_ref[0])
        for sub in range(1, SUBS):
            acc = acc + dot_rows(spread_ref[sub], hot_ref[sub])
        acc_ref[...] += acc
        return 0

    lax.fori_loop(0, steps, step, 0)
    for high, half, block, tile in table_tiles():
        cols = slice(half * 128, half * 128 + 128)
        for part in range(2):
            table_ref[tile_rows(block, tile, 2 * ROWS, ROWS * part), :] = joined(
                acc_ref, 2 * part, high, cols
            )


def image_kernel(
    count_ref, coef_ref, prec_ref, state_ref, pred_ref, chan_ref,
    table_ref, image_ref,
    hot_ref, got_ref, coef_split, spread_ref, acc_ref,
):
    for high, half, block, tile in table_tiles():
        acc_ref[high * 8 : high * 8 + 8, half * 128 : half * 128 + 128] = coef_ref[
            tile_rows(block, tile, ROWS), :
        ]
    high_part, low_part = split(acc_ref[0 : 8 * HIGH, :])
    coef_split[0 : 8 * HIGH, :] = high_part
    coef_split[8 * HIGH :, :] = low_part
    acc_ref[...] = jnp.zeros_like(acc_ref)

    def one_hots(g, sub):
        rows = pl.ds(pl.multiple_of(g * GROUP, GROUP), GROUP)
        one_hot_low(chan_ref[rows, :] & (LOW - 1), hot_ref.at[sub])

    def lookups(g, sub):
        got_ref[sub] = jnp.dot(coef_split[...], hot_ref[sub], preferred_element_type=F32)

    def images(g, sub):
        rows = pl.ds(pl.multiple_of(g * GROUP, GROUP), GROUP)
        high_id = chan_ref[rows, :] >> 8
        got = got_ref.at[sub]
        looked = []
        preds = []
        for j in range(GROUP):
            cols = slice(j * LINE, (j + 1) * LINE)
            pred = pred_ref[:, pl.ds(pl.multiple_of(g * KSLOT + j * LINE, LINE), LINE)]
            ids = jnp.broadcast_to(high_id[j : j + 1], (8, LINE))
            coef = [got[at : at + 8, cols] for at in (0, 8 * HIGH)]
            for high in range(1, HIGH):
                mask = ids == high
                coef = [
                    jnp.where(mask, got[at + 8 * high : at + 8 * high + 8, cols], old)
                    for at, old in zip((0, 8 * HIGH), coef)
                ]
            looked.append(jnp.sum(pred * (coef[0] + coef[1]), axis=0, keepdims=True))
            preds.append(pred)
        weight = live_weights(count_ref[0, 0], g, GROUP, prec_ref[rows, :])
        image = weight * (state_ref[rows, :] + jnp.concatenate(looked, axis=0))
        image_ref[rows, :] = image
        high_f = high_id.astype(F32)
        for j in range(GROUP):
            cols = slice(j * LINE, (j + 1) * LINE)
            spread_high(
                [preds[j] * image[j : j + 1]], high_f[j : j + 1], spread_ref.at[sub], cols
            )

    def step(i, _):
        for work in (one_hots, lookups, images):
            for sub in range(SUBS):
                work(i * SUBS + sub, sub)
        acc = dot_rows(spread_ref[0], hot_ref[0])
        for sub in range(1, SUBS):
            acc = acc + dot_rows(spread_ref[sub], hot_ref[sub])
        acc_ref[...] += acc
        return 0

    lax.fori_loop(0, LINES // GROUP // SUBS, step, 0)
    table_ref[...] = jnp.zeros_like(table_ref)
    for high, half, block, tile in table_tiles():
        table_ref[tile_rows(block, tile, ROWS), :] = joined(
            acc_ref, 0, high, slice(half * 128, half * 128 + 128)
        )


def jac_copy(jac_hbm, jac_ref, sems, i):
    at = pl.ds(pl.multiple_of(i * UNROLL * LINE, UNROLL * LINE), UNROLL * LINE)
    return pltpu.make_async_copy(jac_hbm.at[at], jac_ref.at[at], sems.at[i])


def start_jac(*refs):
    for i in range(STAGES):
        jac_copy(*refs, i).start()


def adjoint_kernel(first, *refs):
    if first:
        row_ref, count_ref, col_ref, innov_ref, prec_ref, jac_hbm, field_ref, jac_ref, sems = refs
    else:
        row_ref, col_ref, value_ref, jac_hbm, field_ref, jac_ref, sems = refs
    start_jac(jac_hbm, jac_ref, sems)
    field_ref[...] = jnp.zeros_like(field_ref)
    ids = lax.broadcasted_iota(jnp.int32, (LON_DEV, LINE), 0).astype(F32).astype(BF16)

    def step(g, _):
        jac_copy(jac_hbm, jac_ref, sems, g).wait()
        rows = pl.ds(pl.multiple_of(g * UNROLL, UNROLL), UNROLL)
        col = col_ref[rows, :].astype(F32)
        if first:
            weight = live_weights(count_ref[0, 0], g, UNROLL, prec_ref[rows, :])
            value = weight * innov_ref[rows, :]
        else:
            value = value_ref[rows, :]
        high = value.astype(BF16).astype(F32)
        low = value - high
        for j in range(UNROLL):
            mask = ids == jnp.broadcast_to(col[j : j + 1], (LON_DEV, LINE)).astype(BF16)
            hot = jnp.concatenate(
                [
                    jnp.where(
                        mask,
                        jnp.broadcast_to(part[j : j + 1], (LON_DEV, LINE)).astype(BF16),
                        jnp.zeros((), BF16),
                    )
                    for part in (high, low)
                ],
                axis=0,
            )
            jac = jac_ref[pl.ds(pl.multiple_of(g * UNROLL * LINE + j * LINE, LINE), LINE), :]
            add = jnp.dot(hot, jac, preferred_element_type=F32)
            add = add[:LON_DEV] + add[LON_DEV:]
            at = row_ref[g * UNROLL + j]
            field_ref[at] += add
        return 0

    lax.fori_loop(0, STAGES, step, 0)


def smoothed_row(mid, above, below, smoothing, size):
    left = pltpu.roll(mid, 1, 0)
    right = pltpu.roll(mid, size - 1, 0)
    return mid + smoothing * (above + below + left + right - 4.0 * mid)


WIDE = LON_DEV + 16


def forward_kernel(
    row_ref, edge_ref, field_ref, north_ref, south_ref, west_ref, east_ref, smooth_ref, col_ref, jac_hbm,
    out_hbm, seen_ref,
    jac_ref, sems, out_ref, out_sem, ext_ref, mid_ref, parts_ref,
):
    start_jac(jac_hbm, jac_ref, sems)
    ext_ref[...] = jnp.zeros_like(ext_ref)
    ext_ref[2 : LAT_DEV + 2, 8 : 8 + LON_DEV] = field_ref[...]
    ext_ref[0:2, 8 : 8 + LON_DEV] = north_ref[...]
    ext_ref[LAT_DEV + 2 : LAT_DEV + 4, 8 : 8 + LON_DEV] = south_ref[...]
    ext_ref[:, 6:8] = west_ref[...]
    ext_ref[:, 8 + LON_DEV : 10 + LON_DEV] = east_ref[...]
    smoothing = smooth_ref[...]

    def first(r, _):
        mid_ref[r] = smoothed_row(ext_ref[r + 1], ext_ref[r], ext_ref[r + 2], smoothing, WIDE)
        return 0

    lax.fori_loop(0, LAT_DEV + 2, first, 0, unroll=2)
    mid_ref[0] = mid_ref[0] * jnp.where(edge_ref[0] > 0, 1.0, 0.0)
    mid_ref[LAT_DEV + 1] = mid_ref[LAT_DEV + 1] * jnp.where(edge_ref[1] > 0, 1.0, 0.0)

    def second(r, _):
        mid = mid_ref[r + 1]
        twice = smoothed_row(mid, mid_ref[r], mid_ref[r + 2], smoothing, WIDE)
        out_ref[r] = mid[8 : 8 + LON_DEV]
        high, low = split(twice[8 : 8 + LON_DEV])
        parts_ref[r, 0:LON_DEV, :] = high
        parts_ref[r, LON_DEV:, :] = low
        return 0

    lax.fori_loop(0, LAT_DEV, second, 0, unroll=4)
    out_copy = pltpu.make_async_copy(out_ref, out_hbm, out_sem.at[0])
    out_copy.start()
    ids = lax.broadcasted_iota(jnp.int32, (LON_DEV, LINE), 0)

    def step(g, _):
        jac_copy(jac_hbm, jac_ref, sems, g).wait()
        rows = pl.ds(pl.multiple_of(g * UNROLL, UNROLL), UNROLL)
        col = col_ref[rows, :]
        seen = []
        for j in range(UNROLL):
            jac = jac_ref[pl.ds(pl.multiple_of(g * UNROLL * LINE + j * LINE, LINE), LINE), :]
            at = row_ref[g * UNROLL + j]
            grid = dot_rows(parts_ref[at], jac)
            grid = grid[:LON_DEV] + grid[LON_DEV:]
            mask = ids == jnp.broadcast_to(col[j : j + 1], (LON_DEV, LINE))
            seen.append(jnp.sum(jnp.where(mask, grid, 0.0), axis=0, keepdims=True))
        seen_ref[rows, :] = jnp.concatenate(seen, axis=0)
        return 0

    lax.fori_loop(0, STAGES, step, 0)
    out_copy.wait()


def lanes_of(values):
    lane = lax.broadcasted_iota(jnp.int32, (1, 128), 1)
    row = jnp.zeros((1, 128), F32)
    for i, value in enumerate(values):
        row = jnp.where(lane == i, value, row)
    return row


def total(x):
    return jnp.sum(jnp.sum(x, axis=0, keepdims=True), axis=1, keepdims=True)


def state_sums_kernel(
    field_ref, north_ref, south_ref, west_ref, east_ref, smooth_ref,
    count_ref, innov_ref, prec_ref, image1_ref, image2_ref, seen1_ref, seen2_ref,
    sums_ref,
    ext_ref,
):
    ext_ref[...] = jnp.zeros_like(ext_ref)
    ext_ref[1 : LAT_DEV + 1, 8 : 8 + LON_DEV] = field_ref[...]
    ext_ref[0:1, 8 : 8 + LON_DEV] = north_ref[...]
    ext_ref[LAT_DEV + 1 : LAT_DEV + 2, 8 : 8 + LON_DEV] = south_ref[...]
    ext_ref[1 : LAT_DEV + 1, 7:8] = west_ref[...]
    ext_ref[1 : LAT_DEV + 1, 8 + LON_DEV : 9 + LON_DEV] = east_ref[...]
    smoothing = smooth_ref[...]

    def first(r, acc):
        row = smoothed_row(ext_ref[r + 1], ext_ref[r], ext_ref[r + 2], smoothing, WIDE)
        row = row[8 : 8 + LON_DEV]
        return acc + row * row

    acc = lax.fori_loop(0, LAT_DEV, first, jnp.zeros((LON_DEV, LEV), F32))
    source = live_weights(count_ref[0, 0], 0, LINES, prec_ref[...]) * innov_ref[...]
    image1, image2 = (image1_ref[...], image2_ref[...])
    seen1, seen2 = (seen1_ref[...], seen2_ref[...])
    sums_ref[...] = lanes_of(
        [
            total(seen1 * source),
            total(seen1 * image1),
            total(seen2 * image1),
            total(seen1 * image2),
            total(seen2 * image2),
            total(acc),
        ]
    )


def arrived_sum(ref, rows):
    acc = ref[0:24, :]
    for g in range(1, ref.shape[0] // 24):
        acc = acc + ref[24 * g : 24 * g + 24, :]
    out = acc[0:rows]
    for s in range(1, 24 // rows):
        out = out + acc[rows * s : rows * s + rows]
    return out


def to_everyone(rows, ref):
    tile = jnp.concatenate([rows] * (24 // rows.shape[0]), axis=0)
    for g in range(ref.shape[0] // 24):
        ref[24 * g : 24 * g + 24, :] = tile


def owner_start_kernel(arrived_ref, prior_ref, out_ref, own_ref):
    both = arrived_sum(arrived_ref, 2 * ROWS)
    res = both[:ROWS]
    diag = both[ROWS:] + prior_ref[...]
    pre = res / diag
    own_ref[0:3] = res
    own_ref[3:6] = pre
    own_ref[6:9] = diag
    to_everyone(pre, out_ref)


def owner_next_kernel(arrived_ref, prior_ref, own_ref, out_ref, next_ref):
    image = arrived_sum(arrived_ref, ROWS) + prior_ref[...] * own_ref[3:6]
    pre = image / own_ref[6:9]
    next_ref[0:3] = image
    next_ref[3:6] = pre
    to_everyone(pre, out_ref)


def owner_last_kernel(arrived_ref, prior_ref, own_ref, next_ref, sums_ref, out_ref):
    res, pre = (own_ref[0:3], own_ref[3:6])
    image, image_pre = (next_ref[0:3], next_ref[3:6])
    last = arrived_sum(arrived_ref, ROWS) + prior_ref[...] * image_pre
    row = lanes_of(
        [jnp.zeros((1, 1), F32)] * 6
        + [
            total(res * pre),
            total(res * res),
            total(pre * image),
            total(image * image_pre),
            total(res * image),
            total(image * image),
            total(image_pre * last),
            total(res * last),
            total(image * last),
            total(last * last),
        ]
    )
    out_ref[...] = jnp.broadcast_to(row + sums_ref[...], out_ref.shape)


def finish_kernel(chan_ref, arrived_ref, a_ref, b_ref, pre_ref, image_pre_ref, x_ref, bias_ref, norm_ref):
    sums = jnp.sum(arrived_ref[...], axis=0, keepdims=True)
    lane = lax.broadcasted_iota(jnp.int32, (1, 128), 1)
    pick = [
        jnp.sum(jnp.where(lane == i, sums, 0.0), axis=1, keepdims=True) for i in range(16)
    ]
    aa, ab, bb, ac, bc, cc = pick[:6]
    rz_b, rr_b, zq_b, qw_b, rq_b, qq_b, wt_b, rt_b, qt_b, tt_b = pick[6:]
    state_qq = aa + 2.0 * ab + bb
    state_qc = ac + bc
    rz0 = aa + rz_b
    rr0 = aa + rr_b
    zq = aa + ab + zq_b
    qw = state_qq + qw_b
    rq = aa + ab + rq_b
    qq = state_qq + qq_b
    wt = state_qq + state_qc + wt_b
    rt = aa + ab + ac + rt_b
    qt = state_qq + state_qc + qt_b
    tt = state_qq + 2.0 * state_qc + cc + tt_b
    alpha0 = rz0 / zq
    rz1 = rz0 - 2.0 * alpha0 * zq + alpha0 * alpha0 * qw
    rr1 = rr0 - 2.0 * alpha0 * rq + alpha0 * alpha0 * qq
    beta = rz1 / rz0
    grow = 1.0 + beta
    pq = grow * grow * zq - 2.0 * alpha0 * grow * qw + alpha0 * alpha0 * wt
    alpha1 = rz1 / pq
    along = alpha0 + alpha1 * grow
    back = alpha0 * alpha1
    rr2 = (
        rr0
        - 2.0 * along * rq
        + 2.0 * back * rt
        + along * along * qq
        - 2.0 * along * back * qt
        + back * back * tt
    )
    for i, value in enumerate((rr0, rr1, rr2)):
        norm_ref[i] = jnp.sqrt(jnp.maximum(value, 0.0))[0, 0]
    coef_a = along - back
    x_ref[...] = coef_a[None] * a_ref[...] - back[None] * b_ref[...]
    block = chan_ref[0]
    for i in range(2 * CHAN_HIGH):
        rows = tile_rows(block, i, ROWS)
        bias_ref[:, 128 * i : 128 * i + 128] = along * pre_ref[rows, :] - back * image_pre_ref[rows, :]


def exchange(array, width):
    moved = lax.all_to_all(
        array.reshape(DEVICES, 1, width), SWATH_CHAN, split_axis=0, concat_axis=0, tiled=True
    )
    return moved.reshape(array.shape)


def halo(field, width):
    bands = lax.axis_size(SWATH)
    sectors = lax.axis_size("chan")
    north = lax.ppermute(field[LAT_DEV - width :], SWATH, [(i, i + 1) for i in range(bands - 1)])
    south = lax.ppermute(field[:width], SWATH, [(i + 1, i) for i in range(bands - 1)])

    def columns(part):
        if width == 1:
            return part(field)
        return jnp.concatenate([part(north), part(field), part(south)], axis=0)

    ring = [(i, (i + 1) % sectors) for i in range(sectors)]
    west = lax.ppermute(columns(lambda f: f[:, LON_DEV - width :]), "chan", ring)
    east = lax.ppermute(columns(lambda f: f[:, :width]), "chan", [(b, a) for a, b in ring])
    return north, south, west, east


def shape(*dims):
    return jax.ShapeDtypeStruct(dims, F32)


FIELD = shape(LAT_DEV, LON_DEV, LEV)
SQUARE = shape(LINES, LINE)


def run_table_start(count, innov, prec, pred, chan):
    return call(
        table_start_kernel,
        shape(2 * TABLE, 128),
        [SMEM] + [HBM] * 4,
        (count, innov, prec, pred, chan),
        [
            pltpu.VMEM((LINES, LINE), F32),
            pltpu.VMEM((LINES, LINE), F32),
            pltpu.VMEM((NPRED, SLOTS), F32),
            pltpu.VMEM((LINES, LINE), jnp.int32),
            pltpu.SemaphoreType.DMA((3 + LINES // GROUP // SUBS,)),
            pltpu.VMEM((SUBS, LOW, KSLOT), BF16),
            pltpu.VMEM((SUBS, 32 * HIGH, KSLOT), BF16),
            pltpu.VMEM((32 * HIGH, LOW), F32),
        ],
        flops=4 * 10**9,
        limit=24,
        name="table_start",
    )


JAC_STAGES = [pltpu.VMEM((SLOTS, LEV), BF16), pltpu.SemaphoreType.DMA((STAGES,))]


def run_adjoint(line_row, col, values, jac):
    first = len(values) > 1
    return call(
        functools.partial(adjoint_kernel, first),
        FIELD,
        [SMEM, SMEM] + [VMEM] * 3 + [HBM] if first else [SMEM, VMEM, VMEM, HBM],
        (line_row, values[0], col, *values[1:], jac) if first else (line_row, col, *values, jac),
        JAC_STAGES,
        flops=2 * 10**9,
        limit=14,
        name="adjoint",
    )


def run_forward(line_row, edges, field, halos, smooth, col, jac):
    return call(
        forward_kernel,
        (pltpu.HBM((LAT_DEV, LON_DEV, LEV), F32), SQUARE),
        [SMEM, SMEM] + [VMEM] * 7 + [HBM],
        (line_row, edges, field, *halos, smooth, col, jac),
        JAC_STAGES
        + [
            pltpu.VMEM((LAT_DEV, LON_DEV, LEV), F32),
            pltpu.SemaphoreType.DMA((1,)),
            pltpu.VMEM((LAT_DEV + 4, WIDE, LEV), F32),
            pltpu.VMEM((LAT_DEV + 2, WIDE, LEV), F32),
            pltpu.VMEM((LAT_DEV, 2 * LON_DEV, LEV), BF16),
        ],
        flops=2 * 10**9,
        limit=14,
        outs=(HBM, VMEM),
        name="forward",
    )


def run_image(count, coefs, prec, state, pred, chan):
    return call(
        image_kernel,
        (shape(TABLE, 128), SQUARE),
        [SMEM] + [VMEM] * 5,
        (count, coefs, prec, state, pred, chan),
        [
            pltpu.VMEM((SUBS, LOW, KSLOT), BF16),
            pltpu.VMEM((SUBS, 16 * HIGH, KSLOT), F32),
            pltpu.VMEM((16 * HIGH, LOW), BF16),
            pltpu.VMEM((SUBS, 16 * HIGH, KSLOT), BF16),
            pltpu.VMEM((16 * HIGH, LOW), F32),
        ],
        flops=4 * 10**9,
        limit=16,
        name="image",
    )


def body(
    innovations,
    obs_precision,
    jacobian,
    predictors,
    obs_column,
    obs_channel,
    obs_count,
    smoothing,
    bias_precision,
):
    band = lax.axis_index(SWATH)
    sector = lax.axis_index("chan")
    square = (LINES, LINE)
    chan = obs_channel.reshape(square)
    col_all = obs_column.reshape(square)
    line_row = col_all[:, 0] // LON_DEV
    col = col_all % LON_DEV
    smooth = smoothing.reshape(1, LEV)
    edges = jnp.stack([band > 0, band < lax.axis_size(SWATH) - 1]).astype(jnp.int32)
    prior = bias_precision.reshape(NPRED, 2 * CHAN_HIGH, 128).transpose(1, 0, 2).reshape(-1, 128)
    prior = jnp.pad(prior, ((0, 16), (0, 0)), constant_values=1.0)
    prior = lax.dynamic_index_in_dim(prior.reshape(ROWS, -1, 128), band, axis=1, keepdims=False)
    innov = innovations.reshape(square)
    prec = obs_precision.reshape(square)
    jacobian = pltpu.with_memory_space_constraint(jacobian, pltpu.HBM)
    table0 = run_table_start(
        obs_count, *(pltpu.with_memory_space_constraint(x, pltpu.HBM) for x in (innov, prec, predictors, chan))
    )

    def adjoint(*values):
        return run_adjoint(line_row, col, values, jacobian)

    def forward(field):
        return run_forward(line_row, edges, field, halo(field, 2), smooth, col, jacobian)

    def image_of(coefs, state):
        return run_image(obs_count, coefs, prec, state, predictors, chan)

    arrived0 = exchange(table0, 2 * ROWS * 128)
    send0, own = call(
        owner_start_kernel, (shape(TABLE, 128), shape(9, 128)), [VMEM] * 2, (arrived0, prior), limit=3, name="owner_start"
    )
    pre = exchange(send0, ROWS * 128)
    a_field, seen1 = forward(adjoint(obs_count, innov, prec))
    table1, image1 = image_of(pre, seen1)
    arrived1 = exchange(table1, ROWS * 128)
    send1, own_next = call(
        owner_next_kernel, (shape(TABLE, 128), shape(6, 128)), [VMEM] * 3, (arrived1, prior, own), limit=3, name="owner_next"
    )
    image_pre = exchange(send1, ROWS * 128)
    b_field, seen2 = forward(adjoint(image1))
    table2, image2 = image_of(image_pre, seen1 + seen2)
    arrived2 = exchange(table2, ROWS * 128)
    last = adjoint(image2)
    sums = call(
        state_sums_kernel,
        shape(1, 128),
        [VMEM] * 6 + [SMEM] + [VMEM] * 6,
        (last, *halo(last, 1), smooth, obs_count, innov, prec, image1, image2, seen1, seen2),
        [pltpu.VMEM((LAT_DEV + 2, WIDE, LEV), F32)],
        limit=5, name="state_sums",
    )
    send2 = call(
        owner_last_kernel,
        shape(DEVICES, 128),
        [VMEM] * 5,
        (arrived2, prior, own, own_next, sums),
        limit=3, name="owner_last",
    )
    send2, sector = lax.optimization_barrier((send2, sector.reshape(1)))
    arrived3 = exchange(send2, 128)
    state, bias, norms = call(
        finish_kernel,
        (FIELD, shape(NPRED, 2 * CHAN_HIGH * 128), shape(3)),
        [SMEM] + [VMEM] * 5,
        (sector, arrived3, a_field, b_field, pre, image_pre),
        outs=(VMEM, VMEM, SMEM),
        limit=6, name="finish",
    )
    return state, bias, norms


def solution(mesh):
    torus = Mesh(
        mesh.devices.reshape(4, 4, 2, mesh.shape["chan"]), ("swath_0", "swath_1", "swath_2", "chan")
    )
    placed = (
        P(SWATH_CHAN),
        P(SWATH_CHAN),
        P(SWATH_CHAN, None),
        P(None, SWATH_CHAN),
        P(SWATH_CHAN),
        P(SWATH_CHAN),
        P(SWATH, "chan"),
        P(),
        P(None, "chan"),
    )
    return jax.shard_map(
        body,
        mesh=torus,
        in_specs=placed,
        out_specs=(P(SWATH, "chan", None), P(None, "chan"), P()),
        check_vma=False,
    )
```

```python
import functools

import jax
import jax.numpy as jnp
from jax import lax
from jax.experimental import pallas as pl
from jax.experimental.pallas import tpu as pltpu
from jax.sharding import Mesh
from jax.sharding import PartitionSpec as P

LEV = 128
NPRED = 8
LINE = 128
LAT_DEV = 32
LON_DEV = 64
SLOTS = 16384
LINES = SLOTS // LINE
GROUP = 8
KSLOT = GROUP * LINE
SUBS = 8
UNROLL = 32
STAGES = LINES // UNROLL
LOW = 256
HIGH = 20
CHAN_HIGH = 5
N_BLOCK = 4
OUT_PARTS = 4
ROWS = 3
DEVICES = 128
TABLE = DEVICES * ROWS
SWATH = ("swath_0", "swath_1", "swath_2")
SWATH_CHAN = ("swath_0", "swath_1", "swath_2", "chan")
F32 = jnp.float32
BF16 = jnp.bfloat16

VMEM = pl.BlockSpec(memory_space=pltpu.VMEM)
SMEM = pl.BlockSpec(memory_space=pltpu.SMEM)
HBM = pl.BlockSpec(memory_space=pltpu.HBM)


def call(kernel, out_shape, in_specs, args, scratch=(), flops=10**9, limit=40, name=None, outs=None):
    return pl.pallas_call(
        kernel,
        out_shape=out_shape,
        in_specs=in_specs,
        out_specs=outs or jax.tree.map(lambda _: VMEM, out_shape),
        scratch_shapes=list(scratch),
        compiler_params=pltpu.CompilerParams(vmem_limit_bytes=int(limit * 2**20)),
        cost_estimate=pl.CostEstimate(flops=flops, bytes_accessed=4 * 2**20, transcendentals=0),
        name=name,
    )(*args)


def split(x):
    high = x.astype(BF16)
    return high, (x - high.astype(F32)).astype(BF16)


def table_tiles():
    for high in range(HIGH):
        for half in range(2):
            tile = high % CHAN_HIGH * 2 + half
            yield high, half, high // CHAN_HIGH, tile


def tile_rows(block, tile, rows, offset=0):
    start = N_BLOCK * rows * 8 * (tile % 4) + rows * block + tile // 4 + offset
    return pl.ds(start, 8, stride=N_BLOCK * rows)


def one_hot_low(low8, hot_ref):
    ids = lax.broadcasted_iota(jnp.int32, (LOW, LINE), 0).astype(F32).astype(BF16)
    low = low8.astype(F32)
    for j in range(GROUP):
        row = jnp.broadcast_to(low[j : j + 1], (LOW, LINE)).astype(BF16)
        hot_ref[:, j * LINE : (j + 1) * LINE] = jnp.where(
            ids == row, jnp.ones((), BF16), jnp.zeros((), BF16)
        )


def joined(ref, part, high, cols):
    at = 8 * HIGH * part + 8 * high
    return ref[at : at + 8, cols] + ref[at + 8 * HIGH : at + 8 * HIGH + 8, cols]


def spread_high(values, high_row, spread_ref, cols):
    offset = (lax.broadcasted_iota(jnp.int32, (16, LINE), 0) // 8).astype(F32)
    base = (jnp.broadcast_to(high_row, (16, LINE)) - offset).astype(BF16)
    pieces = []
    for value in values:
        for half in split(value):
            pieces.append(jnp.concatenate([half, half], axis=0))
    for m in range(HIGH // 2):
        mask = base == jnp.array(2 * m, BF16)
        for i, piece in enumerate(pieces):
            at = 8 * HIGH * i + 16 * m
            spread_ref[at : at + 16, cols] = jnp.where(mask, piece, jnp.zeros((), BF16))


def dot_rows(left, right):
    return lax.dot_general(left, right, (((1,), (1,)), ((), ())), preferred_element_type=F32)


def live_weights(count, g, lines, prec):
    slot = (
        g * lines * LINE
        + lax.broadcasted_iota(jnp.int32, (lines, LINE), 0) * LINE
        + lax.broadcasted_iota(jnp.int32, (lines, LINE), 1)
    )
    return jnp.where(slot < count, prec, 0.0)


def jac_copy(jac_hbm, jac_ref, sems, i):
    at = pl.ds(pl.multiple_of(i * UNROLL * LINE, UNROLL * LINE), UNROLL * LINE)
    return pltpu.make_async_copy(jac_hbm.at[at], jac_ref.at[at], sems.at[i])


def start_jac(*refs):
    for i in range(STAGES):
        jac_copy(*refs, i).start()


def add_adjoint(row_ref, col_ref, value_of, jac_hbm, jac_ref, sems, field_ref):
    field_ref[...] = jnp.zeros_like(field_ref)
    ids = lax.broadcasted_iota(jnp.int32, (LON_DEV, LINE), 0).astype(F32).astype(BF16)

    def step(g, _):
        jac_copy(jac_hbm, jac_ref, sems, g).wait()
        rows = pl.ds(pl.multiple_of(g * UNROLL, UNROLL), UNROLL)
        col = col_ref[rows, :].astype(F32)
        value = value_of(g, rows)
        high = value.astype(BF16).astype(F32)
        low = value - high
        for j in range(UNROLL):
            mask = ids == jnp.broadcast_to(col[j : j + 1], (LON_DEV, LINE)).astype(BF16)
            hot = jnp.concatenate(
                [
                    jnp.where(
                        mask,
                        jnp.broadcast_to(part[j : j + 1], (LON_DEV, LINE)).astype(BF16),
                        jnp.zeros((), BF16),
                    )
                    for part in (high, low)
                ],
                axis=0,
            )
            jac = jac_ref[pl.ds(pl.multiple_of(g * UNROLL * LINE + j * LINE, LINE), LINE), :]
            add = jnp.dot(hot, jac, preferred_element_type=F32)
            add = add[:LON_DEV] + add[LON_DEV:]
            at = row_ref[g * UNROLL + j]
            field_ref[at] += add
        return 0

    lax.fori_loop(0, STAGES, step, 0)


def even_band():
    return 1 - lax.axis_index("swath_2")


def store_edges(field_ref, even, pair_ref, next_ref):
    width = pair_ref.shape[0]
    far = (LAT_DEV - width) * even
    pair_ref[...] = field_ref[pl.ds(far, width)]
    next_ref[...] = field_ref[pl.ds(LAT_DEV - width - far, width)]


def table_start_kernel(
    count_ref, innov_hbm, prec_hbm, pred_hbm, chan_hbm, column_hbm, jac_hbm,
    table_hbm, field_ref, pair_ref, next_ref, row_ref, col_ref,
    innov_ref, prec_ref, pred_ref, chan_ref, column_ref, column_smem, sems,
    hot_ref, spread_ref, acc_ref, table_ref, table_sem, jac_ref, jac_sems,
):
    small = [
        pltpu.make_async_copy(source, target, sems.at[i])
        for i, (source, target) in enumerate(
            [
                (chan_hbm, chan_ref),
                (innov_hbm, innov_ref),
                (prec_hbm, prec_ref),
                (column_hbm, column_ref),
                (column_hbm, column_smem),
            ]
        )
    ]

    def large(i):
        at = pl.ds(pl.multiple_of(i * SUBS * KSLOT, SUBS * KSLOT), SUBS * KSLOT)
        return pltpu.make_async_copy(pred_hbm.at[:, at], pred_ref.at[:, at], sems.at[5 + i])

    steps = LINES // GROUP // SUBS
    for copy in small + [large(i) for i in range(steps)]:
        copy.start()
    start_jac(jac_hbm, jac_ref, jac_sems)
    count = count_ref[0, 0]
    acc_ref[...] = jnp.zeros_like(acc_ref)
    table_ref[...] = jnp.zeros_like(table_ref)
    for copy in small:
        copy.wait()

    def prepare(g, sub):
        rows = pl.ds(pl.multiple_of(g * GROUP, GROUP), GROUP)
        weight = live_weights(count, g, GROUP, prec_ref[rows, :])
        source = weight * innov_ref[rows, :]
        chan = chan_ref[rows, :]
        one_hot_low(chan & (LOW - 1), hot_ref.at[sub])
        high = (chan >> 8).astype(F32)
        for j in range(GROUP):
            pred = pred_ref[:, pl.ds(pl.multiple_of(g * KSLOT + j * LINE, LINE), LINE)]
            spread_high(
                [pred * source[j : j + 1], pred * pred * weight[j : j + 1]],
                high[j : j + 1],
                spread_ref.at[sub],
                slice(j * LINE, (j + 1) * LINE),
            )

    def step(i, _):
        large(i).wait()
        for sub in range(SUBS):
            prepare(i * SUBS + sub, sub)
        acc = dot_rows(spread_ref[0], hot_ref[0])
        for sub in range(1, SUBS):
            acc = acc + dot_rows(spread_ref[sub], hot_ref[sub])
        acc_ref[...] += acc
        return 0

    lax.fori_loop(0, steps, step, 0)
    for high, half, block, tile in table_tiles():
        cols = slice(half * 128, half * 128 + 128)
        for part in range(2):
            table_ref[tile_rows(block, tile, 2 * ROWS, ROWS * part), :] = joined(
                acc_ref, 2 * part, high, cols
            )
    written = pltpu.make_async_copy(table_ref, table_hbm, table_sem.at[0])
    written.start()

    col_ref[...] = column_ref[...] & (LON_DEV - 1)

    def rows_of(i, _):
        row_ref[i] = column_smem[i, 0] >> 6
        return 0

    lax.fori_loop(0, LINES, rows_of, 0, unroll=16)

    def value_of(g, rows):
        return live_weights(count, g, UNROLL, prec_ref[rows, :]) * innov_ref[rows, :]

    add_adjoint(row_ref, col_ref, value_of, jac_hbm, jac_ref, jac_sems, field_ref)
    store_edges(field_ref, even_band(), pair_ref, next_ref)
    written.wait()


def image_kernel(
    count_ref, row_ref, coef_ref, prec_ref, state_ref, pred_ref, chan_ref, col_ref, jac_hbm,
    table_hbm, image_ref, field_ref, pair_ref, next_ref,
    hot_ref, got_ref, coef_split, spread_ref, acc_ref, table_ref, table_sem, jac_ref, jac_sems,
):
    start_jac(jac_hbm, jac_ref, jac_sems)
    for high, half, block, tile in table_tiles():
        acc_ref[high * 8 : high * 8 + 8, half * 128 : half * 128 + 128] = coef_ref[
            tile_rows(block, tile, ROWS), :
        ]
    high_part, low_part = split(acc_ref[0 : 8 * HIGH, :])
    coef_split[0 : 8 * HIGH, :] = high_part
    coef_split[8 * HIGH :, :] = low_part
    acc_ref[...] = jnp.zeros_like(acc_ref)

    def one_hots(g, sub):
        rows = pl.ds(pl.multiple_of(g * GROUP, GROUP), GROUP)
        one_hot_low(chan_ref[rows, :] & (LOW - 1), hot_ref.at[sub])

    def lookups(g, sub):
        got_ref[sub] = jnp.dot(coef_split[...], hot_ref[sub], preferred_element_type=F32)

    def images(g, sub):
        rows = pl.ds(pl.multiple_of(g * GROUP, GROUP), GROUP)
        high_id = chan_ref[rows, :] >> 8
        got = got_ref.at[sub]
        looked = []
        preds = []
        for j in range(GROUP):
            cols = slice(j * LINE, (j + 1) * LINE)
            pred = pred_ref[:, pl.ds(pl.multiple_of(g * KSLOT + j * LINE, LINE), LINE)]
            ids = jnp.broadcast_to(high_id[j : j + 1], (8, LINE))
            coef = [got[at : at + 8, cols] for at in (0, 8 * HIGH)]
            for high in range(1, HIGH):
                mask = ids == high
                coef = [
                    jnp.where(mask, got[at + 8 * high : at + 8 * high + 8, cols], old)
                    for at, old in zip((0, 8 * HIGH), coef)
                ]
            looked.append(jnp.sum(pred * (coef[0] + coef[1]), axis=0, keepdims=True))
            preds.append(pred)
        weight = live_weights(count_ref[0, 0], g, GROUP, prec_ref[rows, :])
        image = weight * (state_ref[rows, :] + jnp.concatenate(looked, axis=0))
        image_ref[rows, :] = image
        high_f = high_id.astype(F32)
        for j in range(GROUP):
            cols = slice(j * LINE, (j + 1) * LINE)
            spread_high(
                [preds[j] * image[j : j + 1]], high_f[j : j + 1], spread_ref.at[sub], cols
            )

    def step(i, _):
        for work in (one_hots, lookups, images):
            for sub in range(SUBS):
                work(i * SUBS + sub, sub)
        acc = dot_rows(spread_ref[0], hot_ref[0])
        for sub in range(1, SUBS):
            acc = acc + dot_rows(spread_ref[sub], hot_ref[sub])
        acc_ref[...] += acc
        return 0

    lax.fori_loop(0, LINES // GROUP // SUBS, step, 0)
    table_ref[...] = jnp.zeros_like(table_ref)
    for high, half, block, tile in table_tiles():
        table_ref[tile_rows(block, tile, ROWS), :] = joined(
            acc_ref, 0, high, slice(half * 128, half * 128 + 128)
        )
    written = pltpu.make_async_copy(table_ref, table_hbm, table_sem.at[0])
    written.start()
    add_adjoint(
        row_ref, col_ref, lambda g, rows: image_ref[rows, :], jac_hbm, jac_ref, jac_sems, field_ref
    )
    store_edges(field_ref, even_band(), pair_ref, next_ref)
    written.wait()


def smoothed_row(mid, above, below, smoothing, size):
    left = pltpu.roll(mid, 1, 0)
    right = pltpu.roll(mid, size - 1, 0)
    return mid + smoothing * (above + below + left + right - 4.0 * mid)


WIDE = LON_DEV + 16


def fill_extended(ext_ref, even, field_ref, pair_ref, next_ref, west_ref, east_ref):
    width = pair_ref.shape[0]
    ext_ref[...] = jnp.zeros_like(ext_ref)
    pair_at = (LAT_DEV + width) * even
    next_at = LAT_DEV + width - pair_at
    parts = [
        (pair_ref, pl.ds(pair_at, width), slice(0, width)),
        (field_ref, slice(width, LAT_DEV + width), slice(width, LAT_DEV + width)),
        (next_ref, pl.ds(next_at, width), slice(LAT_DEV + width, LAT_DEV + 2 * width)),
    ]
    corners = west_ref.shape[0] > LAT_DEV
    for ref, rows, side in parts:
        ext_ref[rows, 8 : 8 + LON_DEV] = ref[...]
        if not corners:
            if ref is not field_ref:
                continue
            side = slice(0, LAT_DEV)
        ext_ref[rows, 8 - width : 8] = west_ref[side]
        ext_ref[rows, 8 + LON_DEV : 8 + LON_DEV + width] = east_ref[side]


def forward_kernel(
    bands,
    row_ref, field_ref, pair_ref, next_ref, west_ref, east_ref, smooth_ref, col_ref, jac_hbm,
    out_hbm, seen_ref,
    jac_ref, sems, out_ref, out_sem, ext_ref, mid_ref, parts_ref,
):
    start_jac(jac_hbm, jac_ref, sems)
    fill_extended(ext_ref, even_band(), field_ref, pair_ref, next_ref, west_ref, east_ref)
    smoothing = smooth_ref[...]

    def first(r, _):
        mid_ref[r] = smoothed_row(ext_ref[r + 1], ext_ref[r], ext_ref[r + 2], smoothing, WIDE)
        return 0

    lax.fori_loop(0, LAT_DEV + 2, first, 0, unroll=2)
    band = lax.axis_index(SWATH)
    mid_ref[0] = mid_ref[0] * jnp.where(band > 0, 1.0, 0.0)
    mid_ref[LAT_DEV + 1] = mid_ref[LAT_DEV + 1] * jnp.where(band < bands - 1, 1.0, 0.0)

    def second(r, _):
        mid = mid_ref[r + 1]
        twice = smoothed_row(mid, mid_ref[r], mid_ref[r + 2], smoothing, WIDE)
        out_ref[r] = mid[8 : 8 + LON_DEV]
        high, low = split(twice[8 : 8 + LON_DEV])
        parts_ref[r, 0:LON_DEV, :] = high
        parts_ref[r, LON_DEV:, :] = low
        return 0

    lax.fori_loop(0, LAT_DEV, second, 0, unroll=4)
    out_copy = pltpu.make_async_copy(out_ref, out_hbm, out_sem.at[0])
    out_copy.start()
    ids = lax.broadcasted_iota(jnp.int32, (LON_DEV, LINE), 0)

    def step(g, _):
        jac_copy(jac_hbm, jac_ref, sems, g).wait()
        rows = pl.ds(pl.multiple_of(g * UNROLL, UNROLL), UNROLL)
        col = col_ref[rows, :]
        seen = []
        for j in range(UNROLL):
            jac = jac_ref[pl.ds(pl.multiple_of(g * UNROLL * LINE + j * LINE, LINE), LINE), :]
            at = row_ref[g * UNROLL + j]
            grid = dot_rows(parts_ref[at], jac)
            grid = grid[:LON_DEV] + grid[LON_DEV:]
            mask = ids == jnp.broadcast_to(col[j : j + 1], (LON_DEV, LINE))
            seen.append(jnp.sum(jnp.where(mask, grid, 0.0), axis=0, keepdims=True))
        seen_ref[rows, :] = jnp.concatenate(seen, axis=0)
        return 0

    lax.fori_loop(0, STAGES, step, 0)
    out_copy.wait()


def lanes_of(values):
    lane = lax.broadcasted_iota(jnp.int32, (1, 128), 1)
    row = jnp.zeros((1, 128), F32)
    for i, value in enumerate(values):
        row = jnp.where(lane == i, value, row)
    return row


def total(x):
    return jnp.sum(jnp.sum(x, axis=0, keepdims=True), axis=1, keepdims=True)


def state_sums_kernel(
    field_ref, pair_ref, next_ref, west_ref, east_ref, smooth_ref,
    count_ref, innov_ref, prec_ref, image1_ref, image2_ref, seen1_ref, seen2_ref,
    sums_ref,
    ext_ref,
):
    fill_extended(ext_ref, even_band(), field_ref, pair_ref, next_ref, west_ref, east_ref)
    smoothing = smooth_ref[...]

    def first(r, acc):
        row = smoothed_row(ext_ref[r + 1], ext_ref[r], ext_ref[r + 2], smoothing, WIDE)
        row = row[8 : 8 + LON_DEV]
        return acc + row * row

    acc = lax.fori_loop(0, LAT_DEV, first, jnp.zeros((LON_DEV, LEV), F32))
    source = live_weights(count_ref[0, 0], 0, LINES, prec_ref[...]) * innov_ref[...]
    image1, image2 = (image1_ref[...], image2_ref[...])
    seen1, seen2 = (seen1_ref[...], seen2_ref[...])
    sums_ref[...] = lanes_of(
        [
            total(seen1 * source),
            total(seen1 * image1),
            total(seen2 * image1),
            total(seen1 * image2),
            total(seen2 * image2),
            total(acc),
        ]
    )


def arrived_sum(ref, rows):
    acc = ref[0:24, :]
    for g in range(1, ref.shape[0] // 24):
        acc = acc + ref[24 * g : 24 * g + 24, :]
    out = acc[0:rows]
    for s in range(1, 24 // rows):
        out = out + acc[rows * s : rows * s + rows]
    return out


def to_everyone(rows, ref):
    tile = jnp.concatenate([rows] * (24 // rows.shape[0]), axis=0)
    for g in range(ref.shape[0] // 24):
        ref[24 * g : 24 * g + 24, :] = tile


def owner_start_kernel(arrived_ref, prior_ref, out_ref, own_ref):
    both = arrived_sum(arrived_ref, 2 * ROWS)
    res = both[:ROWS]
    diag = both[ROWS:] + prior_ref[...]
    pre = res / diag
    own_ref[0:3] = res
    own_ref[3:6] = pre
    own_ref[6:9] = diag
    to_everyone(pre, out_ref)


def owner_next_kernel(arrived_ref, prior_ref, own_ref, out_ref, next_ref):
    image = arrived_sum(arrived_ref, ROWS) + prior_ref[...] * own_ref[3:6]
    pre = image / own_ref[6:9]
    next_ref[0:3] = image
    next_ref[3:6] = pre
    to_everyone(pre, out_ref)


def owner_last_kernel(arrived_ref, prior_ref, own_ref, next_ref, sums_ref, out_ref):
    res, pre = (own_ref[0:3], own_ref[3:6])
    image, image_pre = (next_ref[0:3], next_ref[3:6])
    last = arrived_sum(arrived_ref, ROWS) + prior_ref[...] * image_pre
    row = lanes_of(
        [jnp.zeros((1, 1), F32)] * 6
        + [
            total(res * pre),
            total(res * res),
            total(pre * image),
            total(image * image_pre),
            total(res * image),
            total(image * image),
            total(image_pre * last),
            total(res * last),
            total(image * last),
            total(last * last),
        ]
    )
    out_ref[...] = jnp.broadcast_to(row + sums_ref[...], out_ref.shape)


def finish_kernel(
    chan_ref, arrived_ref, a_hbm, b_hbm, pre_ref, image_pre_ref,
    x_hbm, bias_ref, norm_ref,
    a_ref, b_ref, in_sems, out_sems,
):
    rows_in = LAT_DEV // OUT_PARTS
    sources = ((a_hbm, a_ref), (b_hbm, b_ref))

    def fetch(i, which):
        at = pl.ds(i * rows_in, rows_in)
        source, target = sources[which]
        return pltpu.make_async_copy(source.at[at], target.at[at], in_sems.at[which, i])

    def write(i):
        at = pl.ds(i * rows_in, rows_in)
        return pltpu.make_async_copy(a_ref.at[at], x_hbm.at[at], out_sems.at[i])

    for i in range(OUT_PARTS):
        for which in range(2):
            fetch(i, which).start()
    sums = jnp.sum(arrived_ref[...], axis=0, keepdims=True)
    lane = lax.broadcasted_iota(jnp.int32, (1, 128), 1)
    pick = [
        jnp.sum(jnp.where(lane == i, sums, 0.0), axis=1, keepdims=True) for i in range(16)
    ]
    aa, ab, bb, ac, bc, cc = pick[:6]
    rz_b, rr_b, zq_b, qw_b, rq_b, qq_b, wt_b, rt_b, qt_b, tt_b = pick[6:]
    state_qq = aa + 2.0 * ab + bb
    state_qc = ac + bc
    rz0 = aa + rz_b
    rr0 = aa + rr_b
    zq = aa + ab + zq_b
    qw = state_qq + qw_b
    rq = aa + ab + rq_b
    qq = state_qq + qq_b
    wt = state_qq + state_qc + wt_b
    rt = aa + ab + ac + rt_b
    qt = state_qq + state_qc + qt_b
    tt = state_qq + 2.0 * state_qc + cc + tt_b
    alpha0 = rz0 / zq
    rz1 = rz0 - 2.0 * alpha0 * zq + alpha0 * alpha0 * qw
    rr1 = rr0 - 2.0 * alpha0 * rq + alpha0 * alpha0 * qq
    beta = rz1 / rz0
    grow = 1.0 + beta
    pq = grow * grow * zq - 2.0 * alpha0 * grow * qw + alpha0 * alpha0 * wt
    alpha1 = rz1 / pq
    along = alpha0 + alpha1 * grow
    back = alpha0 * alpha1
    rr2 = (
        rr0
        - 2.0 * along * rq
        + 2.0 * back * rt
        + along * along * qq
        - 2.0 * along * back * qt
        + back * back * tt
    )
    for i, value in enumerate((rr0, rr1, rr2)):
        norm_ref[i] = jnp.sqrt(jnp.maximum(value, 0.0))[0, 0]
    coef_a = along - back
    for i in range(OUT_PARTS):
        for which in range(2):
            fetch(i, which).wait()
        at = slice(i * rows_in, (i + 1) * rows_in)
        a_ref[at] = coef_a[None] * a_ref[at] - back[None] * b_ref[at]
        write(i).start()
    block = chan_ref[0]
    for i in range(2 * CHAN_HIGH):
        rows = tile_rows(block, i, ROWS)
        bias_ref[:, 128 * i : 128 * i + 128] = along * pre_ref[rows, :] - back * image_pre_ref[rows, :]
    for i in range(OUT_PARTS):
        write(i).wait()


def exchange(array, width):
    moved = lax.all_to_all(
        array.reshape(DEVICES, 1, width), SWATH_CHAN, split_axis=0, concat_axis=0, tiled=True
    )
    return moved.reshape(array.shape)


def halo(field, pair, following):
    width = pair.shape[0]
    bands = lax.axis_size(SWATH)
    sectors = lax.axis_size("chan")
    same = [(i, i ^ 1) for i in range(bands)]
    other = [(i, i + 1) for i in range(1, bands - 1, 2)]
    pair = lax.ppermute(pair, SWATH, same)
    following = lax.ppermute(following, SWATH, other + [(b, a) for a, b in other])

    def columns(part):
        if width == 1:
            return part(field)
        return jnp.concatenate([part(pair), part(field), part(following)], axis=0)

    ring = [(i, (i + 1) % sectors) for i in range(sectors)]
    west = lax.ppermute(columns(lambda f: f[:, LON_DEV - width :]), "chan", ring)
    east = lax.ppermute(columns(lambda f: f[:, :width]), "chan", [(b, a) for a, b in ring])
    return pair, following, west, east


def shape(*dims):
    return jax.ShapeDtypeStruct(dims, F32)


FIELD = shape(LAT_DEV, LON_DEV, LEV)
SQUARE = shape(LINES, LINE)


JAC_STAGES = [pltpu.VMEM((SLOTS, LEV), BF16), pltpu.SemaphoreType.DMA((STAGES,))]


def edges_of(width):
    return (shape(width, LON_DEV, LEV),) * 2


def run_table_start(count, innov, prec, pred, chan, column, jac):
    square = pltpu.VMEM((LINES, LINE), F32)
    whole = pltpu.VMEM((LINES, LINE), jnp.int32)
    return call(
        table_start_kernel,
        (
            pltpu.HBM((2 * TABLE, 128), F32),
            FIELD,
            *edges_of(2),
            jax.ShapeDtypeStruct((LINES,), jnp.int32),
            jax.ShapeDtypeStruct((LINES, LINE), jnp.int32),
        ),
        [SMEM] + [HBM] * 6,
        (count, innov, prec, pred, chan, column, jac),
        [
            square,
            square,
            pltpu.VMEM((NPRED, SLOTS), F32),
            whole,
            whole,
            pltpu.SMEM((LINES, LINE), jnp.int32),
            pltpu.SemaphoreType.DMA((5 + LINES // GROUP // SUBS,)),
            pltpu.VMEM((SUBS, LOW, KSLOT), BF16),
            pltpu.VMEM((SUBS, 32 * HIGH, KSLOT), BF16),
            pltpu.VMEM((32 * HIGH, LOW), F32),
            pltpu.VMEM((2 * TABLE, 128), F32),
            pltpu.SemaphoreType.DMA((1,)),
        ]
        + JAC_STAGES,
        flops=6 * 10**9,
        limit=32,
        outs=(HBM, VMEM, VMEM, VMEM, SMEM, VMEM),
        name="table_start",
    )


def run_forward(line_row, field, halos, smooth, col, jac):
    return call(
        functools.partial(forward_kernel, lax.axis_size(SWATH)),
        (pltpu.HBM((LAT_DEV, LON_DEV, LEV), F32), SQUARE),
        [SMEM] + [VMEM] * 7 + [HBM],
        (line_row, field, *halos, smooth, col, jac),
        JAC_STAGES
        + [
            pltpu.VMEM((LAT_DEV, LON_DEV, LEV), F32),
            pltpu.SemaphoreType.DMA((1,)),
            pltpu.VMEM((LAT_DEV + 4, WIDE, LEV), F32),
            pltpu.VMEM((LAT_DEV + 2, WIDE, LEV), F32),
            pltpu.VMEM((LAT_DEV, 2 * LON_DEV, LEV), BF16),
        ],
        flops=2 * 10**9,
        limit=14,
        outs=(HBM, VMEM),
        name="forward",
    )


def run_image(count, line_row, coefs, prec, state, pred, chan, col, jac, width):
    return call(
        image_kernel,
        (pltpu.HBM((TABLE, 128), F32), SQUARE, FIELD, *edges_of(width)),
        [SMEM] * 2 + [VMEM] * 6 + [HBM],
        (count, line_row, coefs, prec, state, pred, chan, col, jac),
        [
            pltpu.VMEM((SUBS, LOW, KSLOT), BF16),
            pltpu.VMEM((SUBS, 16 * HIGH, KSLOT), F32),
            pltpu.VMEM((16 * HIGH, LOW), BF16),
            pltpu.VMEM((SUBS, 16 * HIGH, KSLOT), BF16),
            pltpu.VMEM((16 * HIGH, LOW), F32),
            pltpu.VMEM((TABLE, 128), F32),
            pltpu.SemaphoreType.DMA((1,)),
        ]
        + JAC_STAGES,
        flops=6 * 10**9,
        limit=36,
        outs=(HBM, VMEM, VMEM, VMEM, VMEM),
        name="image",
    )


def body(
    innovations,
    obs_precision,
    jacobian,
    predictors,
    obs_column,
    obs_channel,
    obs_count,
    smoothing,
    bias_precision,
):
    band = lax.axis_index(SWATH)
    sector = lax.axis_index("chan")
    square = (LINES, LINE)
    chan = obs_channel.reshape(square)
    smooth = smoothing.reshape(1, LEV)
    prior = bias_precision.reshape(NPRED, 2 * CHAN_HIGH, 128).transpose(1, 0, 2).reshape(-1, 128)
    prior = jnp.pad(prior, ((0, 16), (0, 0)), constant_values=1.0)
    prior = lax.dynamic_index_in_dim(prior.reshape(ROWS, -1, 128), band, axis=1, keepdims=False)
    innov = innovations.reshape(square)
    prec = obs_precision.reshape(square)
    jacobian = pltpu.with_memory_space_constraint(jacobian, pltpu.HBM)
    in_hbm = [
        pltpu.with_memory_space_constraint(x, pltpu.HBM)
        for x in (innov, prec, predictors, chan, obs_column.reshape(square))
    ]
    table0, *start, line_row, col = run_table_start(obs_count, *in_hbm, jacobian)

    def forward(field, *edges):
        return run_forward(line_row, field, halo(field, *edges), smooth, col, jacobian)

    def image_of(coefs, state, width):
        return run_image(
            obs_count, line_row, coefs, prec, state, predictors, chan, col, jacobian, width
        )

    arrived0 = exchange(table0, 2 * ROWS * 128)
    send0, own = call(
        owner_start_kernel, (shape(TABLE, 128), shape(9, 128)), [VMEM] * 2, (arrived0, prior), limit=3, name="owner_start"
    )
    pre = exchange(send0, ROWS * 128)
    a_field, seen1 = forward(*start)
    table1, image1, *first = image_of(pre, seen1, 2)
    arrived1 = exchange(table1, ROWS * 128)
    send1, own_next = call(
        owner_next_kernel, (shape(TABLE, 128), shape(6, 128)), [VMEM] * 3, (arrived1, prior, own), limit=3, name="owner_next"
    )
    image_pre = exchange(send1, ROWS * 128)
    b_field, seen2 = forward(*first)
    table2, image2, *last = image_of(image_pre, seen1 + seen2, 1)
    arrived2 = exchange(table2, ROWS * 128)
    sums = call(
        state_sums_kernel,
        shape(1, 128),
        [VMEM] * 6 + [SMEM] + [VMEM] * 6,
        (last[0], *halo(*last), smooth, obs_count, innov, prec, image1, image2, seen1, seen2),
        [pltpu.VMEM((LAT_DEV + 2, WIDE, LEV), F32)],
        limit=5,
        name="state_sums",
    )
    send2 = call(
        owner_last_kernel,
        shape(DEVICES, 128),
        [VMEM] * 5,
        (arrived2, prior, own, own_next, sums),
        limit=3, name="owner_last",
    )
    send2, sector = lax.optimization_barrier((send2, sector.reshape(1)))
    arrived3 = exchange(send2, 128)
    state, bias, norms = call(
        finish_kernel,
        (FIELD, shape(NPRED, 2 * CHAN_HIGH * 128), shape(3)),
        [SMEM, VMEM, HBM, HBM, VMEM, VMEM],
        (
            sector,
            arrived3,
            pltpu.with_memory_space_constraint(a_field, pltpu.HBM),
            pltpu.with_memory_space_constraint(b_field, pltpu.HBM),
            pre,
            image_pre,
        ),
        [
            pltpu.VMEM((LAT_DEV, LON_DEV, LEV), F32),
            pltpu.VMEM((LAT_DEV, LON_DEV, LEV), F32),
            pltpu.SemaphoreType.DMA((2, OUT_PARTS)),
            pltpu.SemaphoreType.DMA((OUT_PARTS,)),
        ],
        outs=(HBM, VMEM, SMEM),
        limit=6,
        name="finish",
    )
    return state, bias, norms


def solution(mesh):
    torus = Mesh(
        mesh.devices.reshape(4, 4, 2, mesh.shape["chan"]), ("swath_0", "swath_1", "swath_2", "chan")
    )
    placed = (
        P(SWATH_CHAN),
        P(SWATH_CHAN),
        P(SWATH_CHAN, None),
        P(None, SWATH_CHAN),
        P(SWATH_CHAN),
        P(SWATH_CHAN),
        P(SWATH, "chan"),
        P(),
        P(None, "chan"),
    )
    return jax.shard_map(
        body,
        mesh=torus,
        in_specs=placed,
        out_specs=(P(SWATH, "chan", None), P(None, "chan"), P()),
        check_vma=False,
    )
```

```python
import functools

import jax
import jax.numpy as jnp
from jax import lax
from jax.experimental import pallas as pl
from jax.experimental.pallas import tpu as pltpu
from jax.sharding import Mesh
from jax.sharding import PartitionSpec as P

LEV = 128
NPRED = 8
LINE = 128
LAT_DEV = 32
LON_DEV = 64
SLOTS = 16384
LINES = SLOTS // LINE
GROUP = 8
KSLOT = GROUP * LINE
SUBS = 8
UNROLL = 64
STAGES = LINES // UNROLL
LOW = 256
HIGH = 20
CHAN_HIGH = 5
N_BLOCK = 4
OUT_PARTS = 4
ROWS = 3
DEVICES = 128
TABLE = DEVICES * ROWS
SWATH = ("swath_0", "swath_1", "swath_2")
SWATH_CHAN = ("swath_0", "swath_1", "swath_2", "chan")
F32 = jnp.float32
BF16 = jnp.bfloat16

VMEM = pl.BlockSpec(memory_space=pltpu.VMEM)
SMEM = pl.BlockSpec(memory_space=pltpu.SMEM)
HBM = pl.BlockSpec(memory_space=pltpu.HBM)


def call(kernel, out_shape, in_specs, args, scratch=(), flops=10**9, limit=40, name=None, outs=None):
    return pl.pallas_call(
        kernel,
        out_shape=out_shape,
        in_specs=in_specs,
        out_specs=outs or jax.tree.map(lambda _: VMEM, out_shape),
        scratch_shapes=list(scratch),
        compiler_params=pltpu.CompilerParams(vmem_limit_bytes=int(limit * 2**20)),
        cost_estimate=pl.CostEstimate(flops=flops, bytes_accessed=4 * 2**20, transcendentals=0),
        name=name,
    )(*args)


def split(x):
    high = x.astype(BF16)
    return high, (x - high.astype(F32)).astype(BF16)


def table_tiles():
    for high in range(HIGH):
        for half in range(2):
            tile = high % CHAN_HIGH * 2 + half
            yield high, half, high // CHAN_HIGH, tile


def tile_rows(block, tile, rows, offset=0):
    start = N_BLOCK * rows * 8 * (tile % 4) + rows * block + tile // 4 + offset
    return pl.ds(start, 8, stride=N_BLOCK * rows)


def one_hot_low(low8, hot_ref):
    ids = lax.broadcasted_iota(jnp.int32, (LOW, LINE), 0).astype(F32).astype(BF16)
    low = low8.astype(F32)
    for j in range(GROUP):
        row = jnp.broadcast_to(low[j : j + 1], (LOW, LINE)).astype(BF16)
        hot_ref[:, j * LINE : (j + 1) * LINE] = jnp.where(
            ids == row, jnp.ones((), BF16), jnp.zeros((), BF16)
        )


def joined(ref, part, high, cols):
    at = 8 * HIGH * part + 8 * high
    return ref[at : at + 8, cols] + ref[at + 8 * HIGH : at + 8 * HIGH + 8, cols]


def spread_high(values, high_row, spread_ref, cols):
    offset = (lax.broadcasted_iota(jnp.int32, (16, LINE), 0) // 8).astype(F32)
    base = (jnp.broadcast_to(high_row, (16, LINE)) - offset).astype(BF16)
    pieces = []
    for value in values:
        for half in split(value):
            pieces.append(jnp.concatenate([half, half], axis=0))
    for m in range(HIGH // 2):
        mask = base == jnp.array(2 * m, BF16)
        for i, piece in enumerate(pieces):
            at = 8 * HIGH * i + 16 * m
            spread_ref[at : at + 16, cols] = jnp.where(mask, piece, jnp.zeros((), BF16))


def dot_rows(left, right):
    return lax.dot_general(left, right, (((1,), (1,)), ((), ())), preferred_element_type=F32)


def live_weights(count, g, lines, prec):
    slot = (
        g * lines * LINE
        + lax.broadcasted_iota(jnp.int32, (lines, LINE), 0) * LINE
        + lax.broadcasted_iota(jnp.int32, (lines, LINE), 1)
    )
    return jnp.where(slot < count, prec, 0.0)


def jac_copy(jac_hbm, jac_ref, sems, i):
    at = pl.ds(pl.multiple_of(i * UNROLL * LINE, UNROLL * LINE), UNROLL * LINE)
    return pltpu.make_async_copy(jac_hbm.at[at], jac_ref.at[at], sems.at[i])


def start_jac(*refs):
    for i in range(STAGES):
        jac_copy(*refs, i).start()


def add_adjoint(row_ref, col_ref, value_of, jac_hbm, jac_ref, sems, field_ref):
    field_ref[...] = jnp.zeros_like(field_ref)
    ids = lax.broadcasted_iota(jnp.int32, (LON_DEV, LINE), 0).astype(F32).astype(BF16)

    def step(g, _):
        jac_copy(jac_hbm, jac_ref, sems, g).wait()
        rows = pl.ds(pl.multiple_of(g * UNROLL, UNROLL), UNROLL)
        col = col_ref[rows, :].astype(F32)
        value = value_of(g, rows)
        high = value.astype(BF16).astype(F32)
        low = value - high
        for j in range(UNROLL):
            mask = ids == jnp.broadcast_to(col[j : j + 1], (LON_DEV, LINE)).astype(BF16)
            hot = jnp.concatenate(
                [
                    jnp.where(
                        mask,
                        jnp.broadcast_to(part[j : j + 1], (LON_DEV, LINE)).astype(BF16),
                        jnp.zeros((), BF16),
                    )
                    for part in (high, low)
                ],
                axis=0,
            )
            jac = jac_ref[pl.ds(pl.multiple_of(g * UNROLL * LINE + j * LINE, LINE), LINE), :]
            add = jnp.dot(hot, jac, preferred_element_type=F32)
            add = add[:LON_DEV] + add[LON_DEV:]
            at = row_ref[g * UNROLL + j]
            field_ref[at] += add
        return 0

    lax.fori_loop(0, STAGES, step, 0)


def even_band():
    return 1 - lax.axis_index("swath_2")


def store_edges(field_ref, even, pair_ref, next_ref):
    width = pair_ref.shape[0]
    far = (LAT_DEV - width) * even
    pair_ref[...] = field_ref[pl.ds(far, width)]
    next_ref[...] = field_ref[pl.ds(LAT_DEV - width - far, width)]


def table_start_kernel(
    count_ref, innov_hbm, prec_hbm, pred_hbm, chan_hbm, column_hbm, jac_hbm,
    table_hbm, field_ref, pair_ref, next_ref, row_ref, col_ref,
    innov_ref, prec_ref, pred_ref, chan_ref, column_ref, column_smem, sems,
    hot_ref, spread_ref, acc_ref, table_ref, table_sem, jac_ref, jac_sems,
):
    small = [
        pltpu.make_async_copy(source, target, sems.at[i])
        for i, (source, target) in enumerate(
            [
                (chan_hbm, chan_ref),
                (innov_hbm, innov_ref),
                (prec_hbm, prec_ref),
                (column_hbm, column_ref),
                (column_hbm, column_smem),
            ]
        )
    ]

    def large(i):
        at = pl.ds(pl.multiple_of(i * SUBS * KSLOT, SUBS * KSLOT), SUBS * KSLOT)
        return pltpu.make_async_copy(pred_hbm.at[:, at], pred_ref.at[:, at], sems.at[5 + i])

    steps = LINES // GROUP // SUBS
    for copy in small + [large(i) for i in range(steps)]:
        copy.start()
    start_jac(jac_hbm, jac_ref, jac_sems)
    count = count_ref[0, 0]
    acc_ref[...] = jnp.zeros_like(acc_ref)
    table_ref[...] = jnp.zeros_like(table_ref)
    for copy in small:
        copy.wait()

    def prepare(g, sub):
        rows = pl.ds(pl.multiple_of(g * GROUP, GROUP), GROUP)
        weight = live_weights(count, g, GROUP, prec_ref[rows, :])
        source = weight * innov_ref[rows, :]
        chan = chan_ref[rows, :]
        one_hot_low(chan & (LOW - 1), hot_ref.at[sub])
        high = (chan >> 8).astype(F32)
        for j in range(GROUP):
            pred = pred_ref[:, pl.ds(pl.multiple_of(g * KSLOT + j * LINE, LINE), LINE)]
            spread_high(
                [pred * source[j : j + 1], pred * pred * weight[j : j + 1]],
                high[j : j + 1],
                spread_ref.at[sub],
                slice(j * LINE, (j + 1) * LINE),
            )

    def step(i, _):
        large(i).wait()
        for sub in range(SUBS):
            prepare(i * SUBS + sub, sub)
        acc = dot_rows(spread_ref[0], hot_ref[0])
        for sub in range(1, SUBS):
            acc = acc + dot_rows(spread_ref[sub], hot_ref[sub])
        acc_ref[...] += acc
        return 0

    lax.fori_loop(0, steps, step, 0)
    for high, half, block, tile in table_tiles():
        cols = slice(half * 128, half * 128 + 128)
        for part in range(2):
            table_ref[tile_rows(block, tile, 2 * ROWS, ROWS * part), :] = joined(
                acc_ref, 2 * part, high, cols
            )
    written = pltpu.make_async_copy(table_ref, table_hbm, table_sem.at[0])
    written.start()

    col_ref[...] = column_ref[...] & (LON_DEV - 1)

    def rows_of(i, _):
        row_ref[i] = column_smem[i, 0] >> 6
        return 0

    lax.fori_loop(0, LINES, rows_of, 0, unroll=16)

    def value_of(g, rows):
        return live_weights(count, g, UNROLL, prec_ref[rows, :]) * innov_ref[rows, :]

    add_adjoint(row_ref, col_ref, value_of, jac_hbm, jac_ref, jac_sems, field_ref)
    store_edges(field_ref, even_band(), pair_ref, next_ref)
    written.wait()


def image_kernel(
    count_ref, row_ref, coef_ref, prec_ref, state_ref, pred_ref, chan_ref, col_ref, jac_hbm,
    table_hbm, image_ref, field_ref, pair_ref, next_ref,
    hot_ref, got_ref, coef_split, spread_ref, acc_ref, table_ref, table_sem, jac_ref, jac_sems,
):
    start_jac(jac_hbm, jac_ref, jac_sems)
    for high, half, block, tile in table_tiles():
        acc_ref[high * 8 : high * 8 + 8, half * 128 : half * 128 + 128] = coef_ref[
            tile_rows(block, tile, ROWS), :
        ]
    high_part, low_part = split(acc_ref[0 : 8 * HIGH, :])
    coef_split[0 : 8 * HIGH, :] = high_part
    coef_split[8 * HIGH :, :] = low_part
    acc_ref[...] = jnp.zeros_like(acc_ref)

    def one_hots(g, sub):
        rows = pl.ds(pl.multiple_of(g * GROUP, GROUP), GROUP)
        one_hot_low(chan_ref[rows, :] & (LOW - 1), hot_ref.at[sub])

    def lookups(g, sub):
        got_ref[sub] = jnp.dot(coef_split[...], hot_ref[sub], preferred_element_type=F32)

    def images(g, sub):
        rows = pl.ds(pl.multiple_of(g * GROUP, GROUP), GROUP)
        high_id = chan_ref[rows, :] >> 8
        got = got_ref.at[sub]
        looked = []
        preds = []
        for j in range(GROUP):
            cols = slice(j * LINE, (j + 1) * LINE)
            pred = pred_ref[:, pl.ds(pl.multiple_of(g * KSLOT + j * LINE, LINE), LINE)]
            ids = jnp.broadcast_to(high_id[j : j + 1], (8, LINE))
            coef = [got[at : at + 8, cols] for at in (0, 8 * HIGH)]
            for high in range(1, HIGH):
                mask = ids == high
                coef = [
                    jnp.where(mask, got[at + 8 * high : at + 8 * high + 8, cols], old)
                    for at, old in zip((0, 8 * HIGH), coef)
                ]
            looked.append(jnp.sum(pred * (coef[0] + coef[1]), axis=0, keepdims=True))
            preds.append(pred)
        weight = live_weights(count_ref[0, 0], g, GROUP, prec_ref[rows, :])
        image = weight * (state_ref[rows, :] + jnp.concatenate(looked, axis=0))
        image_ref[rows, :] = image
        high_f = high_id.astype(F32)
        for j in range(GROUP):
            cols = slice(j * LINE, (j + 1) * LINE)
            spread_high(
                [preds[j] * image[j : j + 1]], high_f[j : j + 1], spread_ref.at[sub], cols
            )

    def step(i, _):
        for work in (one_hots, lookups, images):
            for sub in range(SUBS):
                work(i * SUBS + sub, sub)
        acc = dot_rows(spread_ref[0], hot_ref[0])
        for sub in range(1, SUBS):
            acc = acc + dot_rows(spread_ref[sub], hot_ref[sub])
        acc_ref[...] += acc
        return 0

    lax.fori_loop(0, LINES // GROUP // SUBS, step, 0)
    table_ref[...] = jnp.zeros_like(table_ref)
    for high, half, block, tile in table_tiles():
        table_ref[tile_rows(block, tile, ROWS), :] = joined(
            acc_ref, 0, high, slice(half * 128, half * 128 + 128)
        )
    written = pltpu.make_async_copy(table_ref, table_hbm, table_sem.at[0])
    written.start()
    add_adjoint(
        row_ref, col_ref, lambda g, rows: image_ref[rows, :], jac_hbm, jac_ref, jac_sems, field_ref
    )
    store_edges(field_ref, even_band(), pair_ref, next_ref)
    written.wait()


def smoothed_row(mid, above, below, smoothing, size):
    left = pltpu.roll(mid, 1, 0)
    right = pltpu.roll(mid, size - 1, 0)
    return mid + smoothing * (above + below + left + right - 4.0 * mid)


WIDE = LON_DEV + 16


def fill_extended(ext_ref, even, field_ref, pair_ref, next_ref, west_ref, east_ref):
    width = pair_ref.shape[0]
    ext_ref[...] = jnp.zeros_like(ext_ref)
    pair_at = (LAT_DEV + width) * even
    next_at = LAT_DEV + width - pair_at
    parts = [
        (pair_ref, pl.ds(pair_at, width), slice(0, width)),
        (field_ref, slice(width, LAT_DEV + width), slice(width, LAT_DEV + width)),
        (next_ref, pl.ds(next_at, width), slice(LAT_DEV + width, LAT_DEV + 2 * width)),
    ]
    corners = west_ref.shape[0] > LAT_DEV
    for ref, rows, side in parts:
        ext_ref[rows, 8 : 8 + LON_DEV] = ref[...]
        if not corners:
            if ref is not field_ref:
                continue
            side = slice(0, LAT_DEV)
        ext_ref[rows, 8 - width : 8] = west_ref[side]
        ext_ref[rows, 8 + LON_DEV : 8 + LON_DEV + width] = east_ref[side]


def forward_kernel(
    bands,
    row_ref, field_ref, pair_ref, next_ref, west_ref, east_ref, smooth_ref, col_ref, jac_hbm,
    out_hbm, seen_ref,
    jac_ref, sems, out_ref, out_sem, ext_ref, mid_ref, parts_ref,
):
    start_jac(jac_hbm, jac_ref, sems)
    fill_extended(ext_ref, even_band(), field_ref, pair_ref, next_ref, west_ref, east_ref)
    smoothing = smooth_ref[...]

    def first(r, _):
        mid_ref[r] = smoothed_row(ext_ref[r + 1], ext_ref[r], ext_ref[r + 2], smoothing, WIDE)
        return 0

    lax.fori_loop(0, LAT_DEV + 2, first, 0, unroll=2)
    band = lax.axis_index(SWATH)
    mid_ref[0] = mid_ref[0] * jnp.where(band > 0, 1.0, 0.0)
    mid_ref[LAT_DEV + 1] = mid_ref[LAT_DEV + 1] * jnp.where(band < bands - 1, 1.0, 0.0)

    def second(r, _):
        mid = mid_ref[r + 1]
        twice = smoothed_row(mid, mid_ref[r], mid_ref[r + 2], smoothing, WIDE)
        out_ref[r] = mid[8 : 8 + LON_DEV]
        high, low = split(twice[8 : 8 + LON_DEV])
        parts_ref[r, 0:LON_DEV, :] = high
        parts_ref[r, LON_DEV:, :] = low
        return 0

    lax.fori_loop(0, LAT_DEV, second, 0, unroll=4)
    out_copy = pltpu.make_async_copy(out_ref, out_hbm, out_sem.at[0])
    out_copy.start()
    ids = lax.broadcasted_iota(jnp.int32, (LON_DEV, LINE), 0)

    def step(g, _):
        jac_copy(jac_hbm, jac_ref, sems, g).wait()
        rows = pl.ds(pl.multiple_of(g * UNROLL, UNROLL), UNROLL)
        col = col_ref[rows, :]
        seen = []
        for j in range(UNROLL):
            jac = jac_ref[pl.ds(pl.multiple_of(g * UNROLL * LINE + j * LINE, LINE), LINE), :]
            at = row_ref[g * UNROLL + j]
            grid = dot_rows(parts_ref[at], jac)
            grid = grid[:LON_DEV] + grid[LON_DEV:]
            mask = ids == jnp.broadcast_to(col[j : j + 1], (LON_DEV, LINE))
            seen.append(jnp.sum(jnp.where(mask, grid, 0.0), axis=0, keepdims=True))
        seen_ref[rows, :] = jnp.concatenate(seen, axis=0)
        return 0

    lax.fori_loop(0, STAGES, step, 0)
    out_copy.wait()


def lanes_of(values):
    lane = lax.broadcasted_iota(jnp.int32, (1, 128), 1)
    row = jnp.zeros((1, 128), F32)
    for i, value in enumerate(values):
        row = jnp.where(lane == i, value, row)
    return row


def total(x):
    return jnp.sum(jnp.sum(x, axis=0, keepdims=True), axis=1, keepdims=True)


def state_sums_kernel(
    field_ref, pair_ref, next_ref, west_ref, east_ref, smooth_ref,
    count_ref, innov_ref, prec_ref, image1_ref, image2_ref, seen1_ref, seen2_ref,
    sums_ref,
    ext_ref,
):
    fill_extended(ext_ref, even_band(), field_ref, pair_ref, next_ref, west_ref, east_ref)
    smoothing = smooth_ref[...]

    def first(r, acc):
        row = smoothed_row(ext_ref[r + 1], ext_ref[r], ext_ref[r + 2], smoothing, WIDE)
        row = row[8 : 8 + LON_DEV]
        return acc + row * row

    acc = lax.fori_loop(0, LAT_DEV, first, jnp.zeros((LON_DEV, LEV), F32))
    source = live_weights(count_ref[0, 0], 0, LINES, prec_ref[...]) * innov_ref[...]
    image1, image2 = (image1_ref[...], image2_ref[...])
    seen1, seen2 = (seen1_ref[...], seen2_ref[...])
    sums_ref[...] = lanes_of(
        [
            total(seen1 * source),
            total(seen1 * image1),
            total(seen2 * image1),
            total(seen1 * image2),
            total(seen2 * image2),
            total(acc),
        ]
    )


def arrived_sum(ref, rows):
    acc = ref[0:24, :]
    for g in range(1, ref.shape[0] // 24):
        acc = acc + ref[24 * g : 24 * g + 24, :]
    out = acc[0:rows]
    for s in range(1, 24 // rows):
        out = out + acc[rows * s : rows * s + rows]
    return out


def to_everyone(rows, ref):
    tile = jnp.concatenate([rows] * (24 // rows.shape[0]), axis=0)
    for g in range(ref.shape[0] // 24):
        ref[24 * g : 24 * g + 24, :] = tile


def owner_start_kernel(arrived_ref, prior_ref, out_ref, own_ref):
    both = arrived_sum(arrived_ref, 2 * ROWS)
    res = both[:ROWS]
    diag = both[ROWS:] + prior_ref[...]
    pre = res / diag
    own_ref[0:3] = res
    own_ref[3:6] = pre
    own_ref[6:9] = diag
    to_everyone(pre, out_ref)


def owner_next_kernel(arrived_ref, prior_ref, own_ref, out_ref, next_ref):
    image = arrived_sum(arrived_ref, ROWS) + prior_ref[...] * own_ref[3:6]
    pre = image / own_ref[6:9]
    next_ref[0:3] = image
    next_ref[3:6] = pre
    to_everyone(pre, out_ref)


def owner_last_kernel(arrived_ref, prior_ref, own_ref, next_ref, sums_ref, out_ref):
    res, pre = (own_ref[0:3], own_ref[3:6])
    image, image_pre = (next_ref[0:3], next_ref[3:6])
    last = arrived_sum(arrived_ref, ROWS) + prior_ref[...] * image_pre
    row = lanes_of(
        [jnp.zeros((1, 1), F32)] * 6
        + [
            total(res * pre),
            total(res * res),
            total(pre * image),
            total(image * image_pre),
            total(res * image),
            total(image * image),
            total(image_pre * last),
            total(res * last),
            total(image * last),
            total(last * last),
        ]
    )
    out_ref[...] = jnp.broadcast_to(row + sums_ref[...], out_ref.shape)


def finish_kernel(
    chan_ref, arrived_ref, a_hbm, b_hbm, pre_ref, image_pre_ref,
    x_hbm, bias_ref, norm_ref,
    a_ref, b_ref, in_sems, out_sems,
):
    rows_in = LAT_DEV // OUT_PARTS
    sources = ((a_hbm, a_ref), (b_hbm, b_ref))

    def fetch(i, which):
        at = pl.ds(i * rows_in, rows_in)
        source, target = sources[which]
        return pltpu.make_async_copy(source.at[at], target.at[at], in_sems.at[which, i])

    def write(i):
        at = pl.ds(i * rows_in, rows_in)
        return pltpu.make_async_copy(a_ref.at[at], x_hbm.at[at], out_sems.at[i])

    for i in range(OUT_PARTS):
        for which in range(2):
            fetch(i, which).start()
    sums = jnp.sum(arrived_ref[...], axis=0, keepdims=True)
    lane = lax.broadcasted_iota(jnp.int32, (1, 128), 1)
    pick = [
        jnp.sum(jnp.where(lane == i, sums, 0.0), axis=1, keepdims=True) for i in range(16)
    ]
    aa, ab, bb, ac, bc, cc = pick[:6]
    rz_b, rr_b, zq_b, qw_b, rq_b, qq_b, wt_b, rt_b, qt_b, tt_b = pick[6:]
    state_qq = aa + 2.0 * ab + bb
    state_qc = ac + bc
    rz0 = aa + rz_b
    rr0 = aa + rr_b
    zq = aa + ab + zq_b
    qw = state_qq + qw_b
    rq = aa + ab + rq_b
    qq = state_qq + qq_b
    wt = state_qq + state_qc + wt_b
    rt = aa + ab + ac + rt_b
    qt = state_qq + state_qc + qt_b
    tt = state_qq + 2.0 * state_qc + cc + tt_b
    alpha0 = rz0 / zq
    rz1 = rz0 - 2.0 * alpha0 * zq + alpha0 * alpha0 * qw
    rr1 = rr0 - 2.0 * alpha0 * rq + alpha0 * alpha0 * qq
    beta = rz1 / rz0
    grow = 1.0 + beta
    pq = grow * grow * zq - 2.0 * alpha0 * grow * qw + alpha0 * alpha0 * wt
    alpha1 = rz1 / pq
    along = alpha0 + alpha1 * grow
    back = alpha0 * alpha1
    rr2 = (
        rr0
        - 2.0 * along * rq
        + 2.0 * back * rt
        + along * along * qq
        - 2.0 * along * back * qt
        + back * back * tt
    )
    for i, value in enumerate((rr0, rr1, rr2)):
        norm_ref[i] = jnp.sqrt(jnp.maximum(value, 0.0))[0, 0]
    coef_a = along - back
    for i in range(OUT_PARTS):
        for which in range(2):
            fetch(i, which).wait()
        at = slice(i * rows_in, (i + 1) * rows_in)
        a_ref[at] = coef_a[None] * a_ref[at] - back[None] * b_ref[at]
        write(i).start()
    block = chan_ref[0]
    for i in range(2 * CHAN_HIGH):
        rows = tile_rows(block, i, ROWS)
        bias_ref[:, 128 * i : 128 * i + 128] = along * pre_ref[rows, :] - back * image_pre_ref[rows, :]
    for i in range(OUT_PARTS):
        write(i).wait()


def exchange(array, width):
    moved = lax.all_to_all(
        array.reshape(DEVICES, 1, width), SWATH_CHAN, split_axis=0, concat_axis=0, tiled=True
    )
    return moved.reshape(array.shape)


def halo(field, pair, following):
    width = pair.shape[0]
    bands = lax.axis_size(SWATH)
    sectors = lax.axis_size("chan")
    same = [(i, i ^ 1) for i in range(bands)]
    other = [(i, i + 1) for i in range(1, bands - 1, 2)]
    pair = lax.ppermute(pair, SWATH, same)
    following = lax.ppermute(following, SWATH, other + [(b, a) for a, b in other])

    def columns(part):
        if width == 1:
            return part(field)
        return jnp.concatenate([part(pair), part(field), part(following)], axis=0)

    ring = [(i, (i + 1) % sectors) for i in range(sectors)]
    west = lax.ppermute(columns(lambda f: f[:, LON_DEV - width :]), "chan", ring)
    east = lax.ppermute(columns(lambda f: f[:, :width]), "chan", [(b, a) for a, b in ring])
    return pair, following, west, east


def shape(*dims):
    return jax.ShapeDtypeStruct(dims, F32)


FIELD = shape(LAT_DEV, LON_DEV, LEV)
SQUARE = shape(LINES, LINE)


JAC_STAGES = [pltpu.VMEM((SLOTS, LEV), BF16), pltpu.SemaphoreType.DMA((STAGES,))]


def edges_of(width):
    return (shape(width, LON_DEV, LEV),) * 2


def run_table_start(count, innov, prec, pred, chan, column, jac):
    square = pltpu.VMEM((LINES, LINE), F32)
    whole = pltpu.VMEM((LINES, LINE), jnp.int32)
    return call(
        table_start_kernel,
        (
            pltpu.HBM((2 * TABLE, 128), F32),
            FIELD,
            *edges_of(2),
            jax.ShapeDtypeStruct((LINES,), jnp.int32),
            jax.ShapeDtypeStruct((LINES, LINE), jnp.int32),
        ),
        [SMEM] + [HBM] * 6,
        (count, innov, prec, pred, chan, column, jac),
        [
            square,
            square,
            pltpu.VMEM((NPRED, SLOTS), F32),
            whole,
            whole,
            pltpu.SMEM((LINES, LINE), jnp.int32),
            pltpu.SemaphoreType.DMA((5 + LINES // GROUP // SUBS,)),
            pltpu.VMEM((SUBS, LOW, KSLOT), BF16),
            pltpu.VMEM((SUBS, 32 * HIGH, KSLOT), BF16),
            pltpu.VMEM((32 * HIGH, LOW), F32),
            pltpu.VMEM((2 * TABLE, 128), F32),
            pltpu.SemaphoreType.DMA((1,)),
        ]
        + JAC_STAGES,
        flops=6 * 10**9,
        limit=32,
        outs=(HBM, VMEM, VMEM, VMEM, SMEM, VMEM),
        name="table_start",
    )


def run_forward(line_row, field, halos, smooth, col, jac):
    return call(
        functools.partial(forward_kernel, lax.axis_size(SWATH)),
        (pltpu.HBM((LAT_DEV, LON_DEV, LEV), F32), SQUARE),
        [SMEM] + [VMEM] * 7 + [HBM],
        (line_row, field, *halos, smooth, col, jac),
        JAC_STAGES
        + [
            pltpu.VMEM((LAT_DEV, LON_DEV, LEV), F32),
            pltpu.SemaphoreType.DMA((1,)),
            pltpu.VMEM((LAT_DEV + 4, WIDE, LEV), F32),
            pltpu.VMEM((LAT_DEV + 2, WIDE, LEV), F32),
            pltpu.VMEM((LAT_DEV, 2 * LON_DEV, LEV), BF16),
        ],
        flops=2 * 10**9,
        limit=14,
        outs=(HBM, VMEM),
        name="forward",
    )


def run_image(count, line_row, coefs, prec, state, pred, chan, col, jac, width):
    return call(
        image_kernel,
        (pltpu.HBM((TABLE, 128), F32), SQUARE, FIELD, *edges_of(width)),
        [SMEM] * 2 + [VMEM] * 6 + [HBM],
        (count, line_row, coefs, prec, state, pred, chan, col, jac),
        [
            pltpu.VMEM((SUBS, LOW, KSLOT), BF16),
            pltpu.VMEM((SUBS, 16 * HIGH, KSLOT), F32),
            pltpu.VMEM((16 * HIGH, LOW), BF16),
            pltpu.VMEM((SUBS, 16 * HIGH, KSLOT), BF16),
            pltpu.VMEM((16 * HIGH, LOW), F32),
            pltpu.VMEM((TABLE, 128), F32),
            pltpu.SemaphoreType.DMA((1,)),
        ]
        + JAC_STAGES,
        flops=6 * 10**9,
        limit=36,
        outs=(HBM, VMEM, VMEM, VMEM, VMEM),
        name="image",
    )


def body(
    innovations,
    obs_precision,
    jacobian,
    predictors,
    obs_column,
    obs_channel,
    obs_count,
    smoothing,
    bias_precision,
):
    band = lax.axis_index(SWATH)
    sector = lax.axis_index("chan")
    square = (LINES, LINE)
    chan = obs_channel.reshape(square)
    smooth = smoothing.reshape(1, LEV)
    prior = bias_precision.reshape(NPRED, 2 * CHAN_HIGH, 128).transpose(1, 0, 2).reshape(-1, 128)
    prior = jnp.pad(prior, ((0, 16), (0, 0)), constant_values=1.0)
    prior = lax.dynamic_index_in_dim(prior.reshape(ROWS, -1, 128), band, axis=1, keepdims=False)
    innov = innovations.reshape(square)
    prec = obs_precision.reshape(square)
    jacobian = pltpu.with_memory_space_constraint(jacobian, pltpu.HBM)
    in_hbm = [
        pltpu.with_memory_space_constraint(x, pltpu.HBM)
        for x in (innov, prec, predictors, chan, obs_column.reshape(square))
    ]
    table0, *start, line_row, col = run_table_start(obs_count, *in_hbm, jacobian)

    def forward(field, *edges):
        return run_forward(line_row, field, halo(field, *edges), smooth, col, jacobian)

    def image_of(coefs, state, width):
        return run_image(
            obs_count, line_row, coefs, prec, state, predictors, chan, col, jacobian, width
        )

    arrived0 = exchange(table0, 2 * ROWS * 128)
    send0, own = call(
        owner_start_kernel, (shape(TABLE, 128), shape(9, 128)), [VMEM] * 2, (arrived0, prior), limit=3, name="owner_start"
    )
    pre = exchange(send0, ROWS * 128)
    a_field, seen1 = forward(*start)
    table1, image1, *first = image_of(pre, seen1, 2)
    arrived1 = exchange(table1, ROWS * 128)
    send1, own_next = call(
        owner_next_kernel, (shape(TABLE, 128), shape(6, 128)), [VMEM] * 3, (arrived1, prior, own), limit=3, name="owner_next"
    )
    image_pre = exchange(send1, ROWS * 128)
    b_field, seen2 = forward(*first)
    table2, image2, *last = image_of(image_pre, seen1 + seen2, 1)
    arrived2 = exchange(table2, ROWS * 128)
    sums = call(
        state_sums_kernel,
        shape(1, 128),
        [VMEM] * 6 + [SMEM] + [VMEM] * 6,
        (last[0], *halo(*last), smooth, obs_count, innov, prec, image1, image2, seen1, seen2),
        [pltpu.VMEM((LAT_DEV + 2, WIDE, LEV), F32)],
        limit=5,
        name="state_sums",
    )
    send2 = call(
        owner_last_kernel,
        shape(DEVICES, 128),
        [VMEM] * 5,
        (arrived2, prior, own, own_next, sums),
        limit=3, name="owner_last",
    )
    send2, sector = lax.optimization_barrier((send2, sector.reshape(1)))
    arrived3 = exchange(send2, 128)
    state, bias, norms = call(
        finish_kernel,
        (FIELD, shape(NPRED, 2 * CHAN_HIGH * 128), shape(3)),
        [SMEM, VMEM, HBM, HBM, VMEM, VMEM],
        (
            sector,
            arrived3,
            pltpu.with_memory_space_constraint(a_field, pltpu.HBM),
            pltpu.with_memory_space_constraint(b_field, pltpu.HBM),
            pre,
            image_pre,
        ),
        [
            pltpu.VMEM((LAT_DEV, LON_DEV, LEV), F32),
            pltpu.VMEM((LAT_DEV, LON_DEV, LEV), F32),
            pltpu.SemaphoreType.DMA((2, OUT_PARTS)),
            pltpu.SemaphoreType.DMA((OUT_PARTS,)),
        ],
        outs=(HBM, VMEM, SMEM),
        limit=6,
        name="finish",
    )
    return state, bias, norms


def solution(mesh):
    torus = Mesh(
        mesh.devices.reshape(4, 4, 2, mesh.shape["chan"]), ("swath_0", "swath_1", "swath_2", "chan")
    )
    placed = (
        P(SWATH_CHAN),
        P(SWATH_CHAN),
        P(SWATH_CHAN, None),
        P(None, SWATH_CHAN),
        P(SWATH_CHAN),
        P(SWATH_CHAN),
        P(SWATH, "chan"),
        P(),
        P(None, "chan"),
    )
    return jax.shard_map(
        body,
        mesh=torus,
        in_specs=placed,
        out_specs=(P(SWATH, "chan", None), P(None, "chan"), P()),
        check_vma=False,
    )
```
